256 devices in a mesh: tm: 4 (over x), chan: 64 (over z, y, core).
Axes of the slice: x: 4, y: 4, z: 8, core: 2. Of those that a mesh axis runs over, the one named last changes fastest.
Arguments:
- voltages: bfloat16 [8, 4, 32768, 512], P(None, None, ('tm', 'chan')), may hold values from -6 to 6
- taps: float32 [4, 512], replicated, may hold values from -3 to 3
- busy_mask: int32 [512], replicated, may hold values from 0 to 1, as said below
- drift_low: int32 [512], replicated, may hold values from -16 to 1
Outputs:
- drift_power: float32 [8, 256, 16, 2048], P(None, 'chan', None, 'tm')
The draws below stay inside these ranges and needn't reach their ends.
Inputs may be any that keep to these rules, and one draw needn't show every extreme that they name: `busy_mask`: exactly 256 entries are 1.
All inputs are finite; a program needn't handle non-finite values.
Results may differ from the reference program's by a relative error of at most 0.008.
Values may be sent and summed in bfloat16 or wider, within the bound.
No kernel may reach another device: no remote copies, remote signals or barrier semaphores. Data moves between devices by JAX's collectives and lax.ppermute only.
A program may use at most 128 MiB of HBM per device.

```python
import math
import jax
import jax.numpy as jnp
from jax import lax

COARSE_CHANNELS = 512
FINE = 2048
FA = 32
FB = 64
TAPS = 4
NDRIFT = 16
DSPAN = 16
FSTEP = 4
BEAMS = 8
SPEC = 32768
STEPS = 16
BUSY = 256
N_TM = 4


def draw_busy_mask(key, part):
    perm_key = jax.random.fold_in(key, 11)
    reward_key = jax.random.fold_in(key, 23)
    permuted_order = jax.random.permutation(perm_key, COARSE_CHANNELS).astype(jnp.int32)
    block_reward = jax.random.randint(reward_key, (COARSE_CHANNELS // 8,), 0, 4, dtype=jnp.int32)
    merit_scores = jnp.repeat(block_reward, 8, total_repeat_length=COARSE_CHANNELS) * (2 * COARSE_CHANNELS) + permuted_order
    chosen = lax.top_k(merit_scores, BUSY)[1]
    return jnp.zeros((COARSE_CHANNELS,), jnp.int32).at[chosen].set(1)


def set_ends(drawn, key, low, largest):
    longest = drawn.shape.index(max(drawn.shape))
    spots = []
    for shift in (0, 1):
        where = [jax.random.randint(jax.random.fold_in(key, axis), (), 0, length) for axis, length in enumerate(drawn.shape)]
        where[longest] = (where[longest] + shift) % drawn.shape[longest]
        spots.append(tuple(where))
    return drawn.at[spots[0]].set(low).at[spots[1]].set(largest)


def levels(own_key, extent, cuts, least, high):
    def one(axis_at, shards_of):
        draws = jax.random.uniform(jax.random.fold_in(jax.random.fold_in(own_key, 6), axis_at), (shards_of,), jnp.float32, least / len(cuts), high / len(cuts))
        return jnp.repeat(jnp.exp(draws), extent[axis_at] // shards_of).reshape((-1,) + (1,) * (len(extent) - axis_at - 1))

    factor_of = one(*cuts[0])
    for cut in cuts[1:]:
        factor_of = factor_of * one(*cut)
    return factor_of


def noise(key, dims, spread, most, shards=(), kind=jnp.bfloat16):
    level = levels(key, dims, shards, -0.22, 0.18) if shards else 1.0
    values = jax.random.normal(key, dims, jnp.float32) * spread * level
    return jnp.minimum(jnp.maximum(values, -most), most).astype(kind)


def setup_inputs(seed: int = 0) -> dict:
    keys = jax.random.split(jax.random.key(seed), 5)
    return {
        "voltages": noise(keys[0], (BEAMS, 4, SPEC, COARSE_CHANNELS), 1.0, 6.0, ((2, 256),)),
        "taps": noise(keys[1], (TAPS, COARSE_CHANNELS), 0.5, 3.0, (), jnp.float32),
        "busy_mask": draw_busy_mask(jax.random.fold_in(keys[4], 71), 0),
        "drift_low": set_ends(jax.random.randint(keys[3], (COARSE_CHANNELS,), -DSPAN, DSPAN - NDRIFT + 2), jax.random.fold_in(keys[3], 1), -DSPAN, (DSPAN - NDRIFT + 2) - 1).astype(jnp.int32),
    }


def busy_index(busy_mask, busy_count):
    mask_ints = busy_mask.astype(jnp.int32)
    before = (jnp.cumsum(mask_ints) - mask_ints).astype(jnp.int32)
    slot_ids = jnp.arange(busy_count, dtype=jnp.int32)
    is_slot = (mask_ints[:, None] == 1) & (before[:, None] == slot_ids[None, :])
    positions = jnp.arange(busy_mask.shape[0], dtype=jnp.int32)
    return jnp.sum(jnp.where(is_slot, positions[:, None], 0), axis=0).astype(jnp.int32)


def real_dft(sample_pos, freq_ids, length):
    phase_index = (sample_pos[:, None] * freq_ids[None, :]) % length
    angles = phase_index.astype(jnp.float32) * (2.0 * math.pi / length)
    cosines = jnp.cos(angles)
    sine_table = jnp.sin(angles)
    upper = jnp.stack([cosines, -sine_table], axis=1)
    lower = jnp.stack([sine_table, cosines], axis=1)
    return jnp.stack([upper, lower], axis=0).astype(jnp.bfloat16)


def to_bfloat(values):
    return lax.optimization_barrier(values.astype(jnp.bfloat16)).astype(jnp.float32)


def detect_power(spectra):
    items, lanes, chan_rows, samples = spectra.shape
    step_count = samples // (FA * FB)
    shaped = spectra.reshape(items, 2, 2, chan_rows, step_count, FA, FB).astype(jnp.float32)
    short_ids = jnp.arange(FA, dtype=jnp.int32)
    long_ids = jnp.arange(FB, dtype=jnp.int32)
    first_dft = real_dft(short_ids, short_ids, FA).astype(jnp.float32)
    second_dft = real_dft(long_ids, long_ids, FB).astype(jnp.float32)
    first_pass = jnp.einsum("xopctab,paqf->xoqctfb", shaped, first_dft, precision=lax.Precision.HIGHEST)
    twist = (short_ids[:, None] * long_ids[None, :]) % (FA * FB)
    twist_angles = twist.astype(jnp.float32) * (2.0 * math.pi / (FA * FB))
    twist_cos = jnp.cos(twist_angles)
    twist_sin = jnp.sin(twist_angles)
    real_part = first_pass[:, :, 0]
    imag_part = first_pass[:, :, 1]
    turned = jnp.stack([real_part * twist_cos + imag_part * twist_sin, imag_part * twist_cos - real_part * twist_sin], axis=2).astype(jnp.bfloat16)
    second_pass = jnp.einsum("xoqctfb,qbsg->xosctgf", turned.astype(jnp.float32), second_dft, precision=lax.Precision.HIGHEST)
    powers = jnp.sum(second_pass * second_pass, axis=(1, 2)) / (4.0 * FA * FB)
    return powers.reshape(items, chan_rows, step_count, FA * FB)


def drift_rows(step_rows, first_step, drift_rates, first_bin, bin_width, pad_width):
    padded = jnp.pad(step_rows, ((0, 0), (0, 0), (0, 0), (pad_width, pad_width)))
    chan_rows = step_rows.shape[1]
    chan_pick = jnp.arange(chan_rows, dtype=jnp.int32)[:, None, None]
    start_offsets = jnp.arange(bin_width, dtype=jnp.int32)
    running = jnp.zeros((step_rows.shape[0], chan_rows, drift_rates.shape[1], bin_width), jnp.float32)
    for row_index in range(step_rows.shape[2]):
        step_time = first_step + row_index
        anchor = pad_width + first_bin + drift_rates * step_time
        positions = (anchor[:, :, None] + start_offsets[None, None, :]).astype(jnp.int32)
        picked = padded[:, :, row_index][:, chan_pick, positions]
        running = running + picked
    return running


def reference(voltages, taps, busy_mask, drift_low):
    slot_index = busy_index(busy_mask, BUSY)
    coarse_dft = real_dft(jnp.arange(COARSE_CHANNELS, dtype=jnp.int32), slot_index, COARSE_CHANNELS).astype(jnp.float32)

    def one_beam(beam_volts):
        extended = jnp.pad(beam_volts, ((0, 0), (0, TAPS - 1), (0, 0)))
        filtered = taps[0] * extended[:, 0:SPEC]
        for tap_index in range(1, TAPS):
            filtered = filtered + taps[tap_index] * extended[:, tap_index:tap_index + SPEC]
        filtered = filtered.astype(jnp.bfloat16).astype(jnp.float32).reshape(2, 2, SPEC, COARSE_CHANNELS)
        coarse = jnp.einsum("opsn,pnqr->oqrs", filtered, coarse_dft, precision=lax.Precision.HIGHEST)
        coarse = (coarse * COARSE_CHANNELS ** -0.5).astype(jnp.bfloat16)
        return detect_power(coarse.reshape(1, 4, BUSY, SPEC))[0]

    powers = lax.map(one_beam, voltages)
    low_rates = drift_low[slot_index].astype(jnp.int32)
    drift_rates = (low_rates[:, None] + jnp.arange(NDRIFT, dtype=jnp.int32)[None, :]).astype(jnp.int32)
    pad_width = DSPAN * (STEPS - 1)
    drift_total = jnp.zeros((BEAMS, BUSY, NDRIFT, FINE), jnp.float32)
    for group_index in range(N_TM):
        step_rows = powers[:, :, group_index * FSTEP:(group_index + 1) * FSTEP]
        drift_total = drift_total + to_bfloat(drift_rows(step_rows, group_index * FSTEP, drift_rates, 0, FINE, pad_width))
    return drift_total / STEPS
```

```python
import math

import jax
import jax.numpy as jnp
import numpy as np
from jax import lax
from jax.experimental import pallas as pl
from jax.experimental.pallas import tpu as pltpu
from jax.sharding import Mesh, PartitionSpec as P

TAPS = 4
NDRIFT = 16
N = 512
FINE = 2048
BEAMS = 8
STEPS = 16
BLK = 128
GRP = 16
PAD = 256
WIN = 1024
BINS = 512
f32 = jnp.float32
bf16 = jnp.bfloat16


def np_bf16(a):
    return np.asarray(a, np.float32).astype(jnp.bfloat16)


def coarse_tables():
    idx = np.arange(N)
    ang = (idx[:, None] * idx[None, :]) % N * (2.0 * math.pi / N)
    return np_bf16(np.cos(ang)), np_bf16(np.sin(ang))


def fine_tables():
    f1 = np.arange(GRP)
    j = np.arange(BLK)
    ang = (f1[:, None] * j[None, :]) % FINE * (2.0 * math.pi / FINE)
    tw = np.stack([np.cos(ang), np.sin(ang)]).astype(np.float32)
    a2 = (j[:, None] * j[None, :]) % BLK * (2.0 * math.pi / BLK)
    c, s = np.cos(a2), np.sin(a2)
    dft = np.concatenate([np.concatenate([c, -s], 1), np.concatenate([s, c], 1)], 0)
    src = np.arange(256)
    perm = np.zeros((256, 256), np.float32)
    perm[src, src // 16 + 16 * (src % 16)] = 1.0
    return tw, np_bf16(dft), np_bf16(perm)


def coarse_kernel(v_ref, halo_ref, taps_ref, mask_ref, cos_ref, sin_ref, out_ref, wt_ref, filt_ref):
    @pl.when(pl.program_id(0) == 0)
    def _():
        row = lax.broadcasted_iota(jnp.int32, (N, N), 0)
        col = lax.broadcasted_iota(jnp.int32, (N, N), 1)
        upper = (row < col).astype(f32).astype(bf16)
        mask = jnp.broadcast_to(mask_ref[...], (8, N))
        before = jnp.dot(mask.astype(f32).astype(bf16), upper, preferred_element_type=f32)[0:1]
        rp = lax.broadcasted_iota(jnp.int32, (256, N), 0)
        g = rp // 16
        zh = (rp // 4) % 4
        i = rp % 4
        slot = zh * 64 + g * 4 + i
        hit = (before.astype(jnp.int32) == slot) & (mask_ref[...] == 1)
        one_hot = hit.astype(f32).astype(bf16)
        c = jnp.dot(one_hot, cos_ref[...], preferred_element_type=f32)
        s = jnp.dot(one_hot, sin_ref[...], preferred_element_type=f32)
        cb = c.astype(bf16).reshape(GRP, 16, N)
        sb = s.astype(bf16).reshape(GRP, 16, N)
        nb = (-s).astype(bf16).reshape(GRP, 16, N)
        wt_ref[:, 0:16, 0:N] = cb
        wt_ref[:, 0:16, N : 2 * N] = sb
        wt_ref[:, 16:32, 0:N] = nb
        wt_ref[:, 16:32, N : 2 * N] = cb

    for o in range(2):
        for p in range(2):
            for c in range(N // 128):
                lanes = pl.ds(c * 128, 128)
                main = v_ref[0, 2 * o + p, :, lanes].astype(f32)
                tail = halo_ref[0, 2 * o + p, :, lanes].astype(f32)
                ext = jnp.concatenate([main, tail], axis=0)
                acc = taps_ref[0:1, lanes] * main
                for tap in range(1, TAPS):
                    acc = acc + taps_ref[tap : tap + 1, lanes] * ext[tap : tap + BLK]
                filt_ref[pl.ds(o * BLK, BLK), pl.ds(p * N + c * 128, 128)] = acc.astype(bf16)
    res = lax.dot_general(
        wt_ref[...].reshape(2 * 256, 2 * N),
        filt_ref[...],
        (((1,), (1,)), ((), ())),
        preferred_element_type=f32,
    )
    res = (res * (N ** -0.5)).astype(bf16)
    out_ref[...] = res.reshape(GRP, 1, 32, 256)


def coarse(volt, halo, taps, mask, cos_t, sin_t):
    return pl.pallas_call(
        coarse_kernel,
        grid=(BEAMS,),
        in_specs=[
            pl.BlockSpec((1, 4, BLK, N), lambda b: (b, 0, 0, 0)),
            pl.BlockSpec((1, 4, 8, N), lambda b: (b, 0, 0, 0)),
            pl.BlockSpec((TAPS, N), lambda b: (0, 0)),
            pl.BlockSpec((1, N), lambda b: (0, 0)),
            pl.BlockSpec((N, N), lambda b: (0, 0)),
            pl.BlockSpec((N, N), lambda b: (0, 0)),
        ],
        out_specs=pl.BlockSpec((GRP, 1, 32, 256), lambda b: (0, b, 0, 0)),
        out_shape=jax.ShapeDtypeStruct((GRP, BEAMS, 32, 256), bf16),
        scratch_shapes=[pltpu.VMEM((GRP, 32, 2 * N), bf16), pltpu.VMEM((256, 2 * N), bf16)],
        name="coarse",
    )(volt, halo, taps, mask, cos_t, sin_t)


def dft4(x):
    (r0, i0), (r1, i1), (r2, i2), (r3, i3) = x
    ar, ai = r0 + r2, i0 + i2
    br, bi = r0 - r2, i0 - i2
    cr, ci = r1 + r3, i1 + i3
    dr, di = r1 - r3, i1 - i3
    return [(ar + cr, ai + ci), (br + di, bi - dr), (ar - cr, ai - ci), (br - di, bi + dr)]


def turn(x, cos, sin):
    r, i = x
    return r * cos + i * sin, i * cos - r * sin


def fine_kernel(x_ref, tw_ref, dft_ref, perm_ref, out_ref, lhs_ref, pow_ref):
    b = pl.program_id(0)

    @pl.when(b == 0)
    def _():
        pow_ref[:, 0:2, :] = jnp.zeros((128, 2, 128), f32)
        pow_ref[:, 18:20, :] = jnp.zeros((128, 2, 128), f32)

    total = None
    for o in range(2):
        lanes = pl.ds(o * BLK, BLK)
        stage = []
        for m in range(4):
            x = []
            for a in range(4):
                k = 4 * a + m
                x.append((x_ref[k, 0, 0:16, lanes].astype(f32), x_ref[k, 0, 16:32, lanes].astype(f32)))
            y = dft4(x)
            row = []
            for c in range(4):
                if m * c == 0:
                    row.append(y[c])
                else:
                    ang = 2.0 * math.pi * m * c / 16.0
                    row.append(turn(y[c], math.cos(ang), math.sin(ang)))
            stage.append(row)
        for c in range(4):
            y = dft4([stage[m][c] for m in range(4)])
            for d in range(4):
                f1 = c + 4 * d
                if f1 == 0:
                    r, i = y[d]
                else:
                    r, i = turn(y[d], tw_ref[0, f1 : f1 + 1, :], tw_ref[1, f1 : f1 + 1, :])
                lhs_ref[o, f1 * 16 : (f1 + 1) * 16, 0:BLK] = r.astype(bf16)
                lhs_ref[o, f1 * 16 : (f1 + 1) * 16, BLK : 2 * BLK] = i.astype(bf16)
        z = jnp.dot(lhs_ref[o], dft_ref[...], preferred_element_type=f32)
        part = z[:, 0:BLK] * z[:, 0:BLK] + z[:, BLK : 2 * BLK] * z[:, BLK : 2 * BLK]
        total = part if total is None else total + part
    total = total * (1.0 / 8192.0)
    lane = lax.broadcasted_iota(jnp.int32, (16, 128), 1)
    rows = [[None, None] for _ in range(8)]
    for h in range(2):
        v = [total[(8 * h + i) * 16 : (8 * h + i + 1) * 16] for i in range(8)]
        for dist in (4, 2, 1):
            low = (lane // 16) % (2 * dist) < dist
            new = list(v)
            for i in range(8):
                if i & dist == 0:
                    a, e = v[i], v[i + dist]
                    new[i] = jnp.where(low, a, pltpu.roll(e, dist * 16, 1))
                    new[i + dist] = jnp.where(low, pltpu.roll(a, 128 - dist * 16, 1), e)
            v = new
        for m in range(8):
            rows[m][h] = v[m]
    mixed = jnp.concatenate([jnp.concatenate(rows[m], axis=1) for m in range(8)], axis=0).astype(bf16)
    q = jnp.dot(mixed, perm_ref[...], preferred_element_type=f32)
    for m in range(8):
        for h in range(2):
            pow_ref[pl.ds(b, 16, stride=8), 2 + 2 * m + h, :] = q[m * 16 : (m + 1) * 16, h * 128 : (h + 1) * 128]

    @pl.when(b == BEAMS - 1)
    def _():
        for x in range(4):
            for w in range(WIN // 128):
                out_ref[x, :, w * 128 : (w + 1) * 128] = pow_ref[:, 4 * x + w, :].astype(bf16)


def fine(x, tw, dft, perm):
    return pl.pallas_call(
        fine_kernel,
        grid=(BEAMS,),
        in_specs=[
            pl.BlockSpec((GRP, 1, 32, 256), lambda b: (0, b, 0, 0)),
            pl.BlockSpec((2, GRP, BLK), lambda b: (0, 0, 0)),
            pl.BlockSpec((256, 256), lambda b: (0, 0)),
            pl.BlockSpec((256, 256), lambda b: (0, 0)),
        ],
        out_specs=pl.BlockSpec((4, 128, WIN), lambda b: (0, 0, 0)),
        out_shape=jax.ShapeDtypeStruct((4, 128, WIN), bf16),
        scratch_shapes=[pltpu.VMEM((2, 256, 256), bf16), pltpu.VMEM((128, 20, 128), f32)],
        name="fine",
    )(x, tw, dft, perm)


def drift_kernel(low_ref, x_ref, out_ref, wide_ref):
    for t in range(STEPS):
        for w in range(WIN // 128):
            wide_ref[t, w] = x_ref[t, :, w * 128 : (w + 1) * 128].astype(f32)
    lane = lax.broadcasted_iota(jnp.int32, (8, 128), 1)

    def body(ij, carry):
        i = ij // NDRIFT
        j = ij % NDRIFT
        d = low_ref[i] + j
        rows = pl.ds(pl.multiple_of(i * 8, 8), 8)
        acc = [None] * 4
        for t in range(STEPS):
            start = PAD + d * t
            base = start // 128
            off = start % 128
            if t == 0:
                w = [wide_ref[t, 2 + k, rows, :] for k in range(4)]
            else:
                r = [pltpu.roll(wide_ref[t, base + k, rows, :], (128 - off) % 128, 1) for k in range(5)]
                keep = lane < 128 - off
                w = [jnp.where(keep, r[k], r[k + 1]) for k in range(4)]
            acc = w if t == 0 else [acc[k] + w[k] for k in range(4)]
        for k in range(4):
            out_ref[pl.ds(i * NDRIFT + j, 8, stride=64), k, :] = acc[k] * (1.0 / STEPS)
        return carry

    lax.fori_loop(0, 4 * NDRIFT, body, 0)


def drift(low, x):
    return pl.pallas_call(
        drift_kernel,
        in_specs=[
            pl.BlockSpec(memory_space=pltpu.SMEM),
            pl.BlockSpec(memory_space=pltpu.VMEM),
        ],
        out_specs=pl.BlockSpec(memory_space=pltpu.VMEM),
        out_shape=jax.ShapeDtypeStruct((BEAMS * 64, 4, 128), f32),
        scratch_shapes=[pltpu.VMEM((STEPS, WIN // 128, 32, 128), f32)],
        name="drift",
    )(low, x)


def own_low_rates(busy_mask, drift_low, first):
    before = jnp.cumsum(busy_mask) - busy_mask
    slots = first + jnp.arange(4, dtype=jnp.int32)
    hit = (busy_mask[None, :] == 1) & (before[None, :] == slots[:, None])
    return jnp.sum(jnp.where(hit, drift_low[None, :], 0), axis=1).astype(jnp.int32)


def shards(voltages, taps, busy_mask, drift_low):
    axes = ("x", "zh", "zl", "y", "core")
    devices = lax.axis_size(axes)
    head = lax.slice_in_dim(voltages, 0, 8, axis=2)
    halo = lax.ppermute(head, axes, [(i + 1, i) for i in range(devices - 1)])
    cos_t, sin_t = coarse_tables()
    tw, dft, perm = fine_tables()
    blocks = coarse(voltages, halo, taps, busy_mask.reshape(1, N), jnp.asarray(cos_t), jnp.asarray(sin_t))
    times = lax.all_to_all(blocks, ("zl", "y", "core"), split_axis=0, concat_axis=0, tiled=True)
    powers = fine(times, jnp.asarray(tw), jnp.asarray(dft), jnp.asarray(perm))
    wins = lax.all_to_all(powers.reshape(16, 32, WIN), ("x", "zh"), split_axis=0, concat_axis=0, tiled=True)
    low = own_low_rates(busy_mask, drift_low, lax.axis_index(("zh", "zl", "y", "core")) * 4)
    out = drift(low, wins)
    return out.reshape(BEAMS, 4, NDRIFT, BINS)


def solution(mesh):
    fold = Mesh(mesh.devices.reshape(4, 4, 2, 4, 2), ("x", "zh", "zl", "y", "core"))
    chan = ("zh", "zl", "y", "core")
    in_specs = (P(None, None, ("x",) + chan, None), P(), P(), P())
    out_specs = P(None, chan, None, "x")
    return jax.shard_map(shards, mesh=fold, in_specs=in_specs, out_specs=out_specs, check_vma=False)
```

```python
import math

import jax
import jax.numpy as jnp
import numpy as np
from jax import lax
from jax.experimental import pallas as pl
from jax.experimental.pallas import tpu as pltpu
from jax.sharding import Mesh, PartitionSpec as P

TAPS = 4
NDRIFT = 16
N = 512
FINE = 2048
BEAMS = 8
STEPS = 16
BLK = 128
GRP = 16
WIN = 768
BINS = 512
BPS = 2
f32 = jnp.float32
bf16 = jnp.bfloat16


def np_bf16(a):
    return np.asarray(a, np.float32).astype(jnp.bfloat16)


def fine_tables():
    k = np.arange(GRP)
    ang = (k[:, None] * k[None, :]) % GRP * (2.0 * math.pi / GRP)
    c, sn = np.cos(ang), np.sin(ang)
    eye = np.eye(16)
    first = np.zeros((GRP, 2, 16, GRP, 2, 16))
    for q, p, val in ((0, 0, c), (0, 1, sn), (1, 0, -sn), (1, 1, c)):
        first[:, q, :, :, p, :] = val[:, None, :, None] * eye[None, :, None, :]
    f1 = np.arange(GRP)
    lane = np.arange(BLK)
    block = (lane[None, :] // 16 - f1[:, None]) % 8
    f2 = block * 16 + lane[None, :] % 16
    j = np.arange(BLK)
    ang = (j[None, :, None] * (f1[:, None] + 16 * f2)[:, None, :]) % FINE * (2.0 * math.pi / FINE)
    c, sn = np.cos(ang), np.sin(ang)
    second = np.concatenate([np.concatenate([c, -sn], 2), np.concatenate([sn, c], 2)], 1)
    perm = np.zeros((256, 256))
    for h in range(2):
        perm[h * 128 + lane, 8 * h + lane // 16 + 16 * (lane % 16)] = 1.0
    return np_bf16(first.reshape(512, 512)), np_bf16(second), np_bf16(perm)


def cos_sin(phase):
    quarter = lax.shift_right_arithmetic(phase + 64, 7)
    x = (phase - quarter * 128).astype(f32) * (2.0 * math.pi / N)
    y = x * x
    c = 1.0 + y * (-0.5 + y * (1.0 / 24 + y * (-1.0 / 720 + y * (1.0 / 40320))))
    s = x * (1.0 + y * (-1.0 / 6 + y * (1.0 / 120 + y * (-1.0 / 5040 + y * (1.0 / 362880)))))
    swap = (quarter & 1) == 1
    cos = jnp.where(swap, s, c)
    sin = jnp.where(swap, c, s)
    cos = jnp.where(((quarter + 1) & 2) == 2, -cos, cos)
    sin = jnp.where((quarter & 2) == 2, -sin, sin)
    return cos, sin


def write_tables(mask_ref, low_ref, wt_ref, rate_ref):
    row = lax.broadcasted_iota(jnp.int32, (N, N), 0)
    col = lax.broadcasted_iota(jnp.int32, (N, N), 1)
    upper = (row < col).astype(f32).astype(bf16)
    mask = jnp.broadcast_to(mask_ref[...], (8, N))
    before = jnp.dot(mask.astype(f32).astype(bf16), upper, preferred_element_type=f32)[0:1].astype(jnp.int32)
    before = jnp.where(mask_ref[...] == 1, before, -1)
    for r0 in range(0, 256, 16):
        rp = r0 + lax.broadcasted_iota(jnp.int32, (16, N), 0)
        pos = lax.broadcasted_iota(jnp.int32, (16, N), 1)
        hit = before == (rp // 4) % 4 * 64 + rp // 16 * 4 + rp % 4
        rate_ref[r0 : r0 + 16] = jnp.sum(jnp.where(hit, low_ref[...], 0), axis=1, keepdims=True)
        chan = jnp.sum(jnp.where(hit, pos, 0), axis=1, keepdims=True)
        cos, sin = cos_sin((chan * pos) & (N - 1))
        wt_ref[r0 // 16, 0:16, 0:N] = cos.astype(bf16)
        wt_ref[r0 // 16, 0:16, N : 2 * N] = sin.astype(bf16)
        wt_ref[r0 // 16, 16:32, 0:N] = (-sin).astype(bf16)
        wt_ref[r0 // 16, 16:32, N : 2 * N] = cos.astype(bf16)


def front_kernel(mask_ref, low_ref, taps_ref, v_ref, wt_ref, rate_ref, filt_ref, ext_ref):
    @pl.when(pl.program_id(0) == 0)
    def _():
        write_tables(mask_ref, low_ref, wt_ref, rate_ref)
        for c in range(N // 128):
            ext_ref[c, BLK : BLK + 8, :] = jnp.zeros((8, 128), f32)

    def body(bo, carry):
        b = bo // 4
        op = bo % 4
        row = pl.multiple_of((op // 2) * BLK, BLK)
        for c in range(N // 128):
            lanes = pl.ds(c * 128, 128)
            main = v_ref[b, op, :, lanes].astype(f32)
            ext_ref[c, 0:BLK, :] = main
            acc = taps_ref[0:1, lanes] * main
            for tap in range(1, TAPS):
                acc = acc + taps_ref[tap : tap + 1, lanes] * ext_ref[c, tap : tap + BLK, :]
            at = pl.multiple_of((op % 2) * N + c * 128, 128)
            filt_ref[b, pl.ds(row, BLK), pl.ds(at, 128)] = acc.astype(bf16)
        return carry

    lax.fori_loop(0, BPS * 4, body, 0)


def front(mask, low, taps, volt):
    whole = lambda shape: pl.BlockSpec(shape, lambda b: (0,) * len(shape))
    return pl.pallas_call(
        front_kernel,
        grid=(BEAMS // BPS,),
        in_specs=[
            whole((1, N)),
            whole((1, N)),
            whole((TAPS, N)),
            pl.BlockSpec((BPS, 4, BLK, N), lambda b: (b, 0, 0, 0)),
        ],
        out_specs=(
            whole((GRP, 32, 2 * N)),
            whole((256, 1)),
            pl.BlockSpec((BPS, 256, 2 * N), lambda b: (b, 0, 0)),
        ),
        out_shape=(
            jax.ShapeDtypeStruct((GRP, 32, 2 * N), bf16),
            jax.ShapeDtypeStruct((256, 1), jnp.int32),
            jax.ShapeDtypeStruct((BEAMS, 256, 2 * N), bf16),
        ),
        scratch_shapes=[pltpu.VMEM((N // 128, BLK + 8, 128), f32)],
        compiler_params=pltpu.CompilerParams(vmem_limit_bytes=57 << 20),
        name="front",
    )(mask, low, taps, volt)


def coarse_kernel(tail_ref, halo_ref, taps_ref, wt_ref, filt_ref, out_ref, buf_ref, ext_ref, res_ref, in_sem, out_sem):
    fetch = [pltpu.make_async_copy(filt_ref.at[b], buf_ref.at[b], in_sem.at[b]) for b in range(BEAMS)]
    send = [pltpu.make_async_copy(res_ref.at[b], out_ref.at[:, b], out_sem.at[b]) for b in range(BEAMS)]
    for copy in fetch:
        copy.start()
    for b in range(BEAMS):
        fetch[b].wait()
        for op in range(4):
            o, p = divmod(op, 2)
            for c in range(N // 128):
                lanes = pl.ds(c * 128, 128)
                slot = (b % 2) * 16 + op * 4 + c
                ext_ref[slot, 0:8, :] = tail_ref[b, op, :, lanes].astype(f32)
                ext_ref[slot, 8:16, :] = halo_ref[b, op, :, lanes].astype(f32)
                acc = taps_ref[0:1, lanes] * ext_ref[slot, 0:8, :]
                for tap in range(1, TAPS):
                    acc = acc + taps_ref[tap : tap + 1, lanes] * ext_ref[slot, tap : tap + 8, :]
                buf_ref[b, (o + 1) * BLK - 8 : (o + 1) * BLK, p * N + c * 128 : p * N + (c + 1) * 128] = acc.astype(bf16)
        for h in range(2):
            half = slice(h * GRP // 2, (h + 1) * GRP // 2)
            res = lax.dot_general(
                wt_ref[half].reshape(256, 2 * N),
                buf_ref[b],
                (((1,), (1,)), ((), ())),
                preferred_element_type=f32,
            )
            res_ref[b, half] = (res * (N ** -0.5)).astype(bf16).reshape(GRP // 2, 32, 256)
        send[b].start()
    for copy in send:
        copy.wait()


def coarse(volt, halo, taps, wt, filt):
    whole = lambda shape: pl.BlockSpec(shape, lambda b: (0,) * len(shape))
    return pl.pallas_call(
        coarse_kernel,
        grid=(1,),
        in_specs=[
            pl.BlockSpec((BEAMS, 4, 8, N), lambda b: (0, 0, BLK // 8 - 1, 0)),
            whole((BEAMS, 4, 8, N)),
            whole((TAPS, N)),
            whole((GRP, 32, 2 * N)),
            pl.BlockSpec(memory_space=pltpu.HBM),
        ],
        out_specs=pl.BlockSpec(memory_space=pltpu.HBM),
        out_shape=jax.ShapeDtypeStruct((GRP, BEAMS, 32, 256), bf16),
        scratch_shapes=[
            pltpu.VMEM((BEAMS, 256, 2 * N), bf16),
            pltpu.VMEM((32, 16, 128), f32),
            pltpu.VMEM((BEAMS, GRP, 32, 256), bf16),
            pltpu.SemaphoreType.DMA((BEAMS,)),
            pltpu.SemaphoreType.DMA((BEAMS,)),
        ],
        compiler_params=pltpu.CompilerParams(vmem_limit_bytes=56 << 20),
        name="coarse",
    )(volt, halo, taps, wt, filt)


def fine_kernel(rate_ref, x_ref, first_ref, second_hbm, perm_ref, out_ref, second_ref, lhs_ref, mix_ref, pow_ref, pow2_ref, sem):
    load = pltpu.make_async_copy(second_hbm, second_ref, sem)
    load.start()

    def beam(b, carry):
        rows = pl.ds(pl.multiple_of(b * 16, 16), 16)
        x = x_ref[:, b].reshape(512, 256)
        for h in range(2):
            y = jnp.dot(first_ref[h * 256 : (h + 1) * 256], x, preferred_element_type=f32).astype(bf16)
            for f in range(8):
                for q in range(2):
                    part = y[(2 * f + q) * 16 : (2 * f + q + 1) * 16]
                    for o in range(2):
                        lhs_ref[8 * h + f, o, rows, q * BLK : (q + 1) * BLK] = part[:, o * BLK : (o + 1) * BLK]
        return carry

    lax.fori_loop(0, BEAMS, beam, 0, unroll=2)
    load.wait()
    for f in range(GRP):
        total = None
        for o in range(2):
            z = jnp.dot(lhs_ref[f, o], second_ref[f], preferred_element_type=f32)
            part = z[:, 0:BLK] * z[:, 0:BLK] + z[:, BLK : 2 * BLK] * z[:, BLK : 2 * BLK]
            total = part if total is None else total + part
        pow2_ref[f] = total * (1.0 / 8192.0)
    lane = lax.broadcasted_iota(jnp.int32, (16, 128), 1)

    def mix(b, carry):
        rows = pl.ds(pl.multiple_of(b * 16, 16), 16)
        for h in range(2):
            v = [pow2_ref[8 * h + i, rows, :] for i in range(8)]
            for bit in (1, 2, 4):
                odd = (lane // (16 * bit)) % 2 == 1
                v = [jnp.where(odd, v[(m + bit) % 8], v[m]) for m in range(8)]
            for m in range(8):
                mix_ref[(8 - m) % 8, rows, h * 128 : (h + 1) * 128] = v[m].astype(bf16)
        return carry

    lax.fori_loop(0, BEAMS, mix, 0, unroll=2)
    zero = jnp.zeros((128, 128), f32)
    for e in (0, 1, 18, 19, 20):
        pow_ref[e] = zero
    for m in range(8):
        spots = [h * BLK + 16 * ((p - m) % 8) for h in range(2) for p in range(8)]
        turned = jnp.concatenate([perm_ref[r : r + 16] for r in spots], axis=0)
        q = jnp.dot(mix_ref[m], turned, preferred_element_type=f32)
        for h in range(2):
            for b in range(BEAMS):
                tile = q[b * 16 : (b + 1) * 16, h * 128 : (h + 1) * 128]
                pow_ref[2 + 2 * m + h, pl.ds(b, 16, stride=8), :] = tile
    low_lane = lax.broadcasted_iota(jnp.int32, (8, 128), 1)
    step = rate_ref[16]

    def shift(ch, carry):
        start = 256 + rate_ref[ch] * step
        base = lax.shift_right_logical(start, 7)
        off = start & 127
        rows = pl.ds(pl.multiple_of(ch * 8, 8), 8)
        last = low_lane >= off
        r = [pow_ref[base + k, rows, :] for k in range(19)]
        for k in range(18):
            pow2_ref[k, rows, :] = pltpu.roll(jnp.where(last, r[k], r[k + 1]), (128 - off) & 127, 1)
        return carry

    lax.fori_loop(0, 16, shift, 0, unroll=4)
    for x in range(4):
        for w in range(WIN // 128):
            out_ref[x, :, w * 128 : (w + 1) * 128] = pow2_ref[4 * x + w].astype(bf16)


def fine(rates, x, first, second, perm):
    vmem = pl.BlockSpec(memory_space=pltpu.VMEM)
    return pl.pallas_call(
        fine_kernel,
        in_specs=[
            pl.BlockSpec(memory_space=pltpu.SMEM),
            vmem,
            vmem,
            pl.BlockSpec(memory_space=pltpu.HBM),
            vmem,
        ],
        out_specs=vmem,
        out_shape=jax.ShapeDtypeStruct((4, 128, WIN), bf16),
        scratch_shapes=[
            pltpu.VMEM((GRP, 256, 256), bf16),
            pltpu.VMEM((GRP, 2, 128, 256), bf16),
            pltpu.VMEM((8, 128, 256), bf16),
            pltpu.VMEM((21, 128, 128), f32),
            pltpu.VMEM((18, 128, 128), f32),
            pltpu.SemaphoreType.DMA,
        ],
        compiler_params=pltpu.CompilerParams(vmem_limit_bytes=56 << 20),
        name="fine",
    )(rates, x, first, second, perm)


def drift_kernel(x_ref, out_ref, wide_ref, sum_ref):
    for t in range(STEPS):
        for w in range(WIN // 128):
            wide_ref[t, w] = x_ref[t, :, w * 128 : (w + 1) * 128].astype(f32)
    lane = lax.broadcasted_iota(jnp.int32, (8, 128), 1)

    def body(i, carry):
        rows = pl.ds(pl.multiple_of(i * 8, 8), 8)
        for j in range(NDRIFT):
            acc = None
            for t in range(STEPS):
                base, off = divmod(j * t, 128)
                if off == 0:
                    w = [wide_ref[t, base + k, rows, :] for k in range(4)]
                else:
                    r = [wide_ref[t, base + k, rows, :] for k in range(5)]
                    w = [pltpu.roll(jnp.where(lane >= off, r[k], r[k + 1]), 128 - off, 1) for k in range(4)]
                acc = w if acc is None else [acc[k] + w[k] for k in range(4)]
            for k in range(4):
                sum_ref[k, pl.ds(i * NDRIFT + j, 8, stride=64), :] = acc[k] * (1.0 / STEPS)
        return carry

    lax.fori_loop(0, 4, body, 0)
    for k in range(4):
        out_ref[:, k * 128 : (k + 1) * 128] = sum_ref[k]


def drift(x):
    return pl.pallas_call(
        drift_kernel,
        in_specs=[pl.BlockSpec(memory_space=pltpu.VMEM)],
        out_specs=pl.BlockSpec(memory_space=pltpu.VMEM),
        out_shape=jax.ShapeDtypeStruct((BEAMS * 64, BINS), f32),
        scratch_shapes=[
            pltpu.VMEM((STEPS, WIN // 128, 32, 128), f32),
            pltpu.VMEM((4, BEAMS * 64, 128), f32),
        ],
        compiler_params=pltpu.CompilerParams(vmem_limit_bytes=56 << 20),
        name="drift",
    )(x)


def shards(voltages, taps, busy_mask, drift_low):
    axes = ("x", "zh", "zl", "y", "core")
    devices = lax.axis_size(axes)
    head = lax.slice_in_dim(voltages, 0, 8, axis=2)
    halo = lax.ppermute(head, axes, [(i + 1, i) for i in range(devices - 1)])
    first, second, perm = fine_tables()
    wt, rates, filt = front(
        busy_mask.reshape(1, N), drift_low.reshape(1, N), taps, voltages
    )
    blocks = coarse(voltages, halo, taps, wt, filt)
    mine = lax.dynamic_slice_in_dim(rates.reshape(256), lax.axis_index(("zl", "y", "core")) * 16, 16)
    step = lax.axis_index(("x", "zh")).astype(jnp.int32).reshape(1)
    rate, blocks = lax.optimization_barrier((jnp.concatenate([mine, step]), blocks))
    times = lax.all_to_all(blocks, ("zl", "y", "core"), split_axis=0, concat_axis=0, tiled=True)
    powers = fine(rate, times, jnp.asarray(first), jnp.asarray(second), jnp.asarray(perm))
    wins = lax.all_to_all(powers.reshape(16, 32, WIN), ("x", "zh"), split_axis=0, concat_axis=0, tiled=True)
    out = drift(wins)
    return out.reshape(BEAMS, 4, NDRIFT, BINS)


def solution(mesh):
    fold = Mesh(mesh.devices.reshape(4, 4, 2, 4, 2), ("x", "zh", "zl", "y", "core"))
    chan = ("zh", "zl", "y", "core")
    in_specs = (P(None, None, ("x",) + chan, None), P(), P(), P())
    out_specs = P(None, chan, None, "x")
    return jax.shard_map(shards, mesh=fold, in_specs=in_specs, out_specs=out_specs, check_vma=False)
```

```python
import math

import jax
import jax.numpy as jnp
import numpy as np
from jax import lax
from jax.experimental import pallas as pl
from jax.experimental.pallas import tpu as pltpu
from jax.sharding import Mesh, PartitionSpec as P

TAPS = 4
NDRIFT = 16
N = 512
FINE = 2048
BEAMS = 8
STEPS = 16
BLK = 128
GRP = 16
WIN = 768
BINS = 512
BPS = 2
f32 = jnp.float32
bf16 = jnp.bfloat16


def np_bf16(a):
    return np.asarray(a, np.float32).astype(jnp.bfloat16)


def fine_tables():
    k = np.arange(GRP)
    ang = (k[:, None] * k[None, :]) % GRP * (2.0 * math.pi / GRP)
    c, sn = np.cos(ang), np.sin(ang)
    eye = np.eye(16)
    first = np.zeros((GRP, 2, 16, GRP, 2, 16))
    for q, p, val in ((0, 0, c), (0, 1, sn), (1, 0, -sn), (1, 1, c)):
        first[:, q, :, :, p, :] = val[:, None, :, None] * eye[None, :, None, :]
    f1 = np.arange(GRP)
    lane = np.arange(BLK)
    block = (lane[None, :] // 16 - f1[:, None]) % 8
    f2 = block * 16 + lane[None, :] % 16
    j = np.arange(BLK)
    ang = (j[None, :, None] * (f1[:, None] + 16 * f2)[:, None, :]) % FINE * (2.0 * math.pi / FINE)
    c, sn = np.cos(ang), np.sin(ang)
    second = np.concatenate([np.concatenate([c, -sn], 2), np.concatenate([sn, c], 2)], 1)
    perm = np.zeros((256, 256))
    for h in range(2):
        perm[h * 128 + lane, 8 * h + lane // 16 + 16 * (lane % 16)] = 1.0
    return np_bf16(first.reshape(512, 512)), np_bf16(second), np_bf16(perm)


def cos_sin(phase):
    quarter = lax.shift_right_arithmetic(phase + 64, 7)
    x = (phase - quarter * 128).astype(f32) * (2.0 * math.pi / N)
    y = x * x
    c = 1.0 + y * (-0.5 + y * (1.0 / 24 + y * (-1.0 / 720 + y * (1.0 / 40320))))
    s = x * (1.0 + y * (-1.0 / 6 + y * (1.0 / 120 + y * (-1.0 / 5040 + y * (1.0 / 362880)))))
    swap = (quarter & 1) == 1
    cos = jnp.where(swap, s, c)
    sin = jnp.where(swap, c, s)
    cos = jnp.where(((quarter + 1) & 2) == 2, -cos, cos)
    sin = jnp.where((quarter & 2) == 2, -sin, sin)
    return cos, sin


def write_tables(small_ref, wt_ref, rate_ref, hit_ref):
    busy = small_ref[TAPS : TAPS + 1]
    row = lax.broadcasted_iota(jnp.int32, (N, N), 0)
    col = lax.broadcasted_iota(jnp.int32, (N, N), 1)
    upper = (row < col).astype(f32).astype(bf16)
    mask = jnp.broadcast_to(busy, (8, N))
    before = jnp.dot(mask.astype(bf16), upper, preferred_element_type=f32)[0:1].astype(jnp.int32)
    before = jnp.where(busy > 0.5, before, -1)
    for r0 in range(0, 256, 16):
        rp = r0 + lax.broadcasted_iota(jnp.int32, (16, N), 0)
        pos = lax.broadcasted_iota(jnp.int32, (16, N), 1)
        hit = before == (rp // 4) % 4 * 64 + rp // 16 * 4 + rp % 4
        hit_ref[r0 : r0 + 16] = hit.astype(f32).astype(bf16)
        chan = jnp.sum(jnp.where(hit, pos, 0), axis=1, keepdims=True)
        cos, sin = cos_sin((chan * pos) & (N - 1))
        wt_ref[r0 // 16, 0:16, 0:N] = cos.astype(bf16)
        wt_ref[r0 // 16, 0:16, N : 2 * N] = sin.astype(bf16)
        wt_ref[r0 // 16, 16:32, 0:N] = (-sin).astype(bf16)
        wt_ref[r0 // 16, 16:32, N : 2 * N] = cos.astype(bf16)
    low = jnp.broadcast_to(small_ref[TAPS + 1 : TAPS + 2], (8, N)).astype(bf16)
    rate = lax.dot_general(low, hit_ref[...], (((1,), (1,)), ((), ())), preferred_element_type=f32)
    rate_ref[...] = rate[0:1].astype(jnp.int32)


def front_kernel(small_ref, v_ref, wt_ref, rate_ref, tail_ref, filt_ref, ext_ref, hit_ref):
    @pl.when(pl.program_id(0) == 0)
    def _():
        write_tables(small_ref, wt_ref, rate_ref, hit_ref)
        for c in range(N // 128):
            ext_ref[c, BLK : BLK + 8, :] = jnp.zeros((8, 128), f32)

    tail_ref[...] = v_ref[:, :, BLK - 8 : BLK, :]

    def body(bo, carry):
        b = bo // 4
        op = bo % 4
        row = pl.multiple_of((op // 2) * BLK, BLK)
        for c in range(N // 128):
            lanes = pl.ds(c * 128, 128)
            main = v_ref[b, op, :, lanes].astype(f32)
            ext_ref[c, 0:BLK, :] = main
            acc = small_ref[0:1, lanes] * main
            for tap in range(1, TAPS):
                acc = acc + small_ref[tap : tap + 1, lanes] * ext_ref[c, tap : tap + BLK, :]
            at = pl.multiple_of((op % 2) * N + c * 128, 128)
            filt_ref[b, pl.ds(row, BLK), pl.ds(at, 128)] = acc.astype(bf16)
        return carry

    lax.fori_loop(0, BPS * 4, body, 0)


def front(small, volt):
    whole = lambda shape: pl.BlockSpec(shape, lambda b: (0,) * len(shape))
    return pl.pallas_call(
        front_kernel,
        grid=(BEAMS // BPS,),
        in_specs=[whole((8, N)), pl.BlockSpec((BPS, 4, BLK, N), lambda b: (b, 0, 0, 0))],
        out_specs=(
            whole((GRP, 32, 2 * N)),
            whole((1, 256)),
            pl.BlockSpec((BPS, 4, 8, N), lambda b: (b, 0, 0, 0)),
            pl.BlockSpec((BPS, 256, 2 * N), lambda b: (b, 0, 0)),
        ),
        out_shape=(
            jax.ShapeDtypeStruct((GRP, 32, 2 * N), bf16),
            jax.ShapeDtypeStruct((1, 256), jnp.int32),
            jax.ShapeDtypeStruct((BEAMS, 4, 8, N), bf16),
            jax.ShapeDtypeStruct((BEAMS, 256, 2 * N), bf16),
        ),
        scratch_shapes=[pltpu.VMEM((N // 128, BLK + 8, 128), f32), pltpu.VMEM((256, N), bf16)],
        compiler_params=pltpu.CompilerParams(vmem_limit_bytes=46 << 20),
        name="front",
    )(small, volt)


def coarse_kernel(tail_ref, halo_ref, taps_ref, wt_ref, filt_ref, out_ref, buf_ref, ext_ref, res_ref, in_sem, out_sem):
    fetch = [pltpu.make_async_copy(filt_ref.at[b], buf_ref.at[b], in_sem.at[b]) for b in range(BEAMS)]
    send = [pltpu.make_async_copy(res_ref.at[b], out_ref.at[:, b], out_sem.at[b]) for b in range(BEAMS)]
    for copy in fetch:
        copy.start()
    for b in range(BEAMS):
        fetch[b].wait()
        for op in range(4):
            o, p = divmod(op, 2)
            for c in range(N // 128):
                lanes = pl.ds(c * 128, 128)
                slot = (b % 2) * 16 + op * 4 + c
                ext_ref[slot, 0:8, :] = tail_ref[b, op, :, lanes].astype(f32)
                ext_ref[slot, 8:16, :] = halo_ref[b, op, :, lanes].astype(f32)
                acc = taps_ref[0:1, lanes] * ext_ref[slot, 0:8, :]
                for tap in range(1, TAPS):
                    acc = acc + taps_ref[tap : tap + 1, lanes] * ext_ref[slot, tap : tap + 8, :]
                buf_ref[b, (o + 1) * BLK - 8 : (o + 1) * BLK, p * N + c * 128 : p * N + (c + 1) * 128] = acc.astype(bf16)
        for h in range(2):
            half = slice(h * GRP // 2, (h + 1) * GRP // 2)
            res = lax.dot_general(
                wt_ref[half].reshape(256, 2 * N),
                buf_ref[b],
                (((1,), (1,)), ((), ())),
                preferred_element_type=f32,
            )
            res_ref[b, half] = (res * (N ** -0.5)).astype(bf16).reshape(GRP // 2, 32, 256)
        send[b].start()
    for copy in send:
        copy.wait()


def coarse(tail, halo, small, wt, filt):
    whole = lambda shape: pl.BlockSpec(shape, lambda b: (0,) * len(shape))
    return pl.pallas_call(
        coarse_kernel,
        grid=(1,),
        in_specs=[
            whole((BEAMS, 4, 8, N)),
            whole((BEAMS, 4, 8, N)),
            whole((8, N)),
            whole((GRP, 32, 2 * N)),
            pl.BlockSpec(memory_space=pltpu.HBM),
        ],
        out_specs=pl.BlockSpec(memory_space=pltpu.HBM),
        out_shape=jax.ShapeDtypeStruct((GRP, BEAMS, 32, 256), bf16),
        scratch_shapes=[
            pltpu.VMEM((BEAMS, 256, 2 * N), bf16),
            pltpu.VMEM((32, 16, 128), f32),
            pltpu.VMEM((BEAMS, GRP, 32, 256), bf16),
            pltpu.SemaphoreType.DMA((BEAMS,)),
            pltpu.SemaphoreType.DMA((BEAMS,)),
        ],
        compiler_params=pltpu.CompilerParams(vmem_limit_bytes=46 << 20),
        name="coarse",
    )(tail, halo, small, wt, filt)


def fine_kernel(rate_ref, x_ref, first_ref, second_hbm, perm_ref, out_ref, second_ref, lhs_ref, mix_ref, pow_ref, pow2_ref, sem):
    load = pltpu.make_async_copy(second_hbm, second_ref, sem)
    load.start()

    def beam(b, carry):
        rows = pl.ds(pl.multiple_of(b * 16, 16), 16)
        x = x_ref[:, b].reshape(512, 256)
        for h in range(2):
            y = jnp.dot(first_ref[h * 256 : (h + 1) * 256], x, preferred_element_type=f32).astype(bf16)
            for f in range(8):
                for q in range(2):
                    part = y[(2 * f + q) * 16 : (2 * f + q + 1) * 16]
                    for o in range(2):
                        lhs_ref[8 * h + f, o, rows, q * BLK : (q + 1) * BLK] = part[:, o * BLK : (o + 1) * BLK]
        return carry

    lax.fori_loop(0, BEAMS, beam, 0, unroll=2)
    load.wait()
    for f in range(GRP):
        total = None
        for o in range(2):
            z = jnp.dot(lhs_ref[f, o], second_ref[f], preferred_element_type=f32)
            part = z[:, 0:BLK] * z[:, 0:BLK] + z[:, BLK : 2 * BLK] * z[:, BLK : 2 * BLK]
            total = part if total is None else total + part
        pow2_ref[f] = total * (1.0 / 8192.0)
    lane = lax.broadcasted_iota(jnp.int32, (16, 128), 1)

    def mix(b, carry):
        rows = pl.ds(pl.multiple_of(b * 16, 16), 16)
        for h in range(2):
            v = [pow2_ref[8 * h + i, rows, :] for i in range(8)]
            for bit in (1, 2, 4):
                odd = (lane // (16 * bit)) % 2 == 1
                v = [jnp.where(odd, v[(m + bit) % 8], v[m]) for m in range(8)]
            for m in range(8):
                mix_ref[(8 - m) % 8, rows, h * 128 : (h + 1) * 128] = v[m].astype(bf16)
        return carry

    lax.fori_loop(0, BEAMS, mix, 0, unroll=2)
    zero = jnp.zeros((128, 128), f32)
    for e in (0, 1, 18, 19, 20):
        pow_ref[e] = zero
    for m in range(8):
        spots = [h * BLK + 16 * ((p - m) % 8) for h in range(2) for p in range(8)]
        turned = jnp.concatenate([perm_ref[r : r + 16] for r in spots], axis=0)
        q = jnp.dot(mix_ref[m], turned, preferred_element_type=f32)
        for h in range(2):
            for b in range(BEAMS):
                tile = q[b * 16 : (b + 1) * 16, h * 128 : (h + 1) * 128]
                pow_ref[2 + 2 * m + h, pl.ds(b, 16, stride=8), :] = tile
    low_lane = lax.broadcasted_iota(jnp.int32, (8, 128), 1)
    step = lax.axis_index(("x", "zh"))
    own = lax.axis_index(("zl", "y", "core")) * 16

    def shift(ch, carry):
        start = 256 + rate_ref[0, own + ch] * step
        base = lax.shift_right_logical(start, 7)
        off = start & 127
        rows = pl.ds(pl.multiple_of(ch * 8, 8), 8)
        last = low_lane >= off
        r = [pow_ref[base + k, rows, :] for k in range(19)]
        for k in range(18):
            pow2_ref[k, rows, :] = pltpu.roll(jnp.where(last, r[k], r[k + 1]), (128 - off) & 127, 1)
        return carry

    lax.fori_loop(0, 16, shift, 0, unroll=4)
    for x in range(4):
        for w in range(WIN // 128):
            out_ref[x, :, w * 128 : (w + 1) * 128] = pow2_ref[4 * x + w].astype(bf16)


def fine(rates, x, first, second, perm):
    vmem = pl.BlockSpec(memory_space=pltpu.VMEM)
    return pl.pallas_call(
        fine_kernel,
        in_specs=[
            pl.BlockSpec(memory_space=pltpu.SMEM),
            vmem,
            vmem,
            pl.BlockSpec(memory_space=pltpu.HBM),
            vmem,
        ],
        out_specs=vmem,
        out_shape=jax.ShapeDtypeStruct((4, 128, WIN), bf16),
        scratch_shapes=[
            pltpu.VMEM((GRP, 256, 256), bf16),
            pltpu.VMEM((GRP, 2, 128, 256), bf16),
            pltpu.VMEM((8, 128, 256), bf16),
            pltpu.VMEM((21, 128, 128), f32),
            pltpu.VMEM((18, 128, 128), f32),
            pltpu.SemaphoreType.DMA,
        ],
        compiler_params=pltpu.CompilerParams(vmem_limit_bytes=50 << 20),
        name="fine",
    )(rates, x, first, second, perm)


def drift_kernel(x_ref, out_ref, wide_ref, sum_ref):
    for t in range(STEPS):
        for w in range(WIN // 128):
            wide_ref[t, w] = x_ref[t, :, w * 128 : (w + 1) * 128].astype(f32)
    lane = lax.broadcasted_iota(jnp.int32, (8, 128), 1)

    def body(i, carry):
        rows = pl.ds(pl.multiple_of(i * 8, 8), 8)
        for j in range(NDRIFT):
            acc = None
            for t in range(STEPS):
                base, off = divmod(j * t, 128)
                if off == 0:
                    w = [wide_ref[t, base + k, rows, :] for k in range(4)]
                else:
                    r = [wide_ref[t, base + k, rows, :] for k in range(5)]
                    w = [pltpu.roll(jnp.where(lane >= off, r[k], r[k + 1]), 128 - off, 1) for k in range(4)]
                acc = w if acc is None else [acc[k] + w[k] for k in range(4)]
            for k in range(4):
                sum_ref[k, pl.ds(i * NDRIFT + j, 8, stride=64), :] = acc[k] * (1.0 / STEPS)
        return carry

    lax.fori_loop(0, 4, body, 0)
    for k in range(4):
        out_ref[:, k * 128 : (k + 1) * 128] = sum_ref[k]


def drift(x):
    return pl.pallas_call(
        drift_kernel,
        in_specs=[pl.BlockSpec(memory_space=pltpu.VMEM)],
        out_specs=pl.BlockSpec(memory_space=pltpu.VMEM),
        out_shape=jax.ShapeDtypeStruct((BEAMS * 64, BINS), f32),
        scratch_shapes=[
            pltpu.VMEM((STEPS, WIN // 128, 32, 128), f32),
            pltpu.VMEM((4, BEAMS * 64, 128), f32),
        ],
        compiler_params=pltpu.CompilerParams(vmem_limit_bytes=50 << 20),
        name="drift",
    )(x)


def shards(voltages, taps, busy_mask, drift_low):
    axes = ("x", "zh", "zl", "y", "core")
    devices = lax.axis_size(axes)
    head = lax.slice_in_dim(voltages, 0, 8, axis=2)
    halo = lax.ppermute(head, axes, [(i + 1, i) for i in range(devices - 1)])
    first, second, perm = fine_tables()
    extra = jnp.stack([busy_mask, drift_low]).astype(f32)
    small = jnp.concatenate([taps, extra, jnp.zeros((2, N), f32)], axis=0)
    wt, rates, tail, filt = front(small, voltages)
    blocks = coarse(tail, halo, small, wt, filt)
    times = lax.all_to_all(blocks, ("zl", "y", "core"), split_axis=0, concat_axis=0, tiled=True)
    powers = fine(rates, times, jnp.asarray(first), jnp.asarray(second), jnp.asarray(perm))
    wins = lax.all_to_all(powers.reshape(16, 32, WIN), ("x", "zh"), split_axis=0, concat_axis=0, tiled=True)
    out = drift(wins)
    return out.reshape(BEAMS, 4, NDRIFT, BINS)


def solution(mesh):
    fold = Mesh(mesh.devices.reshape(4, 4, 2, 4, 2), ("x", "zh", "zl", "y", "core"))
    chan = ("zh", "zl", "y", "core")
    in_specs = (P(None, None, ("x",) + chan, None), P(), P(), P())
    out_specs = P(None, chan, None, "x")
    return jax.shard_map(shards, mesh=fold, in_specs=in_specs, out_specs=out_specs, check_vma=False)
```

```python
import math

import jax
import jax.numpy as jnp
import numpy as np
from jax import lax
from jax.experimental import pallas as pl
from jax.experimental.pallas import tpu as pltpu
from jax.sharding import Mesh, PartitionSpec as P

TAPS = 4
NDRIFT = 16
N = 512
FINE = 2048
BEAMS = 8
STEPS = 16
BLK = 128
GRP = 16
WIN = 768
BINS = 512
BPS = 2
f32 = jnp.float32
bf16 = jnp.bfloat16


def np_bf16(a):
    return np.asarray(a, np.float32).astype(jnp.bfloat16)


def fine_tables():
    k = np.arange(GRP)
    ang = (k[:, None] * k[None, :]) % GRP * (2.0 * math.pi / GRP)
    c, sn = np.cos(ang), np.sin(ang)
    eye = np.eye(16)
    first = np.zeros((GRP, 2, 16, GRP, 2, 16))
    for q, p, val in ((0, 0, c), (0, 1, sn), (1, 0, -sn), (1, 1, c)):
        first[:, q, :, :, p, :] = val[:, None, :, None] * eye[None, :, None, :]
    f1 = np.arange(GRP)
    lane = np.arange(BLK)
    block = (lane[None, :] // 16 - f1[:, None]) % 8
    f2 = block * 16 + lane[None, :] % 16
    j = np.arange(BLK)
    ang = (j[None, :, None] * (f1[:, None] + 16 * f2)[:, None, :]) % FINE * (2.0 * math.pi / FINE)
    c, sn = np.cos(ang), np.sin(ang)
    second = np.concatenate([np.concatenate([c, -sn], 2), np.concatenate([sn, c], 2)], 1)
    perm = np.zeros((256, 256))
    for h in range(2):
        perm[h * 128 + lane, 8 * h + lane // 16 + 16 * (lane % 16)] = 1.0
    return np_bf16(first.reshape(512, 512)), np_bf16(second), np_bf16(perm)


def cos_sin(phase):
    quarter = lax.shift_right_arithmetic(phase + 64, 7)
    x = (phase - quarter * 128).astype(f32) * (2.0 * math.pi / N)
    y = x * x
    c = 1.0 + y * (-0.5 + y * (1.0 / 24 + y * (-1.0 / 720 + y * (1.0 / 40320))))
    s = x * (1.0 + y * (-1.0 / 6 + y * (1.0 / 120 + y * (-1.0 / 5040 + y * (1.0 / 362880)))))
    swap = (quarter & 1) == 1
    cos = jnp.where(swap, s, c)
    sin = jnp.where(swap, c, s)
    cos = jnp.where(((quarter + 1) & 2) == 2, -cos, cos)
    sin = jnp.where((quarter & 2) == 2, -sin, sin)
    return cos, sin


def write_tables(small_ref, wt_ref, rate_ref, hit_ref):
    busy = small_ref[TAPS : TAPS + 1]
    row = lax.broadcasted_iota(jnp.int32, (N, N), 0)
    col = lax.broadcasted_iota(jnp.int32, (N, N), 1)
    upper = (row < col).astype(f32).astype(bf16)
    mask = jnp.broadcast_to(busy, (8, N))
    before = jnp.dot(mask.astype(bf16), upper, preferred_element_type=f32)[0:1].astype(jnp.int32)
    before = jnp.where(busy > 0.5, before, -1)
    for r0 in range(0, 256, 16):
        rp = r0 + lax.broadcasted_iota(jnp.int32, (16, N), 0)
        pos = lax.broadcasted_iota(jnp.int32, (16, N), 1)
        hit = before == (rp // 4) % 4 * 64 + rp // 16 * 4 + rp % 4
        hit_ref[r0 : r0 + 16] = hit.astype(f32).astype(bf16)
        chan = jnp.sum(jnp.where(hit, pos, 0), axis=1, keepdims=True)
        cos, sin = cos_sin((chan * pos[:, 0:BLK]) & (N - 1))
        for c in range(N // BLK):
            turns = (chan * c) & 3
            odd = (turns & 1) == 1
            cos_sign = jnp.where((turns == 1) | (turns == 2), -1.0, 1.0)
            sin_sign = jnp.where(turns >= 2, -1.0, 1.0)
            cc = jnp.where(odd, sin, cos) * cos_sign
            ss = jnp.where(odd, cos, sin) * sin_sign
            lanes = slice(c * BLK, (c + 1) * BLK)
            high = slice(N + c * BLK, N + (c + 1) * BLK)
            wt_ref[r0 // 16, 0:16, lanes] = cc.astype(bf16)
            wt_ref[r0 // 16, 0:16, high] = ss.astype(bf16)
            wt_ref[r0 // 16, 16:32, lanes] = (-ss).astype(bf16)
            wt_ref[r0 // 16, 16:32, high] = cc.astype(bf16)
    low = jnp.broadcast_to(small_ref[TAPS + 1 : TAPS + 2], (8, N)).astype(bf16)
    rate = lax.dot_general(low, hit_ref[...], (((1,), (1,)), ((), ())), preferred_element_type=f32)
    rate_ref[...] = rate[0:1].astype(jnp.int32)


def front_kernel(small_ref, v_ref, wt_ref, rate_ref, tail_ref, filt_ref, ext_ref, hit_ref):
    @pl.when(pl.program_id(0) == 0)
    def _():
        write_tables(small_ref, wt_ref, rate_ref, hit_ref)
        for c in range(N // 128):
            ext_ref[c, BLK : BLK + 8, :] = jnp.zeros((8, 128), f32)

    tail_ref[...] = v_ref[:, :, BLK - 8 : BLK, :]

    def body(bo, carry):
        b = bo // 4
        op = bo % 4
        row = pl.multiple_of((op // 2) * BLK, BLK)
        for c in range(N // 128):
            lanes = pl.ds(c * 128, 128)
            main = v_ref[b, op, :, lanes].astype(f32)
            ext_ref[c, 0:BLK, :] = main
            acc = small_ref[0:1, lanes] * main
            for tap in range(1, TAPS):
                acc = acc + small_ref[tap : tap + 1, lanes] * ext_ref[c, tap : tap + BLK, :]
            at = pl.multiple_of((op % 2) * N + c * 128, 128)
            filt_ref[b, pl.ds(row, BLK), pl.ds(at, 128)] = acc.astype(bf16)
        return carry

    lax.fori_loop(0, BPS * 4, body, 0, unroll=2)


def front(small, volt):
    whole = lambda shape: pl.BlockSpec(shape, lambda b: (0,) * len(shape))
    return pl.pallas_call(
        front_kernel,
        grid=(BEAMS // BPS,),
        in_specs=[whole((8, N)), pl.BlockSpec((BPS, 4, BLK, N), lambda b: (b, 0, 0, 0))],
        out_specs=(
            whole((GRP, 32, 2 * N)),
            whole((1, 256)),
            pl.BlockSpec((BPS, 4, 8, N), lambda b: (b, 0, 0, 0)),
            pl.BlockSpec((BPS, 256, 2 * N), lambda b: (b, 0, 0)),
        ),
        out_shape=(
            jax.ShapeDtypeStruct((GRP, 32, 2 * N), bf16),
            jax.ShapeDtypeStruct((1, 256), jnp.int32),
            jax.ShapeDtypeStruct((BEAMS, 4, 8, N), bf16),
            jax.ShapeDtypeStruct((BEAMS, 256, 2 * N), bf16),
        ),
        scratch_shapes=[pltpu.VMEM((N // 128, BLK + 8, 128), f32), pltpu.VMEM((256, N), bf16)],
        compiler_params=pltpu.CompilerParams(vmem_limit_bytes=46 << 20),
        name="front",
    )(small, volt)


def coarse_kernel(tail_ref, halo_ref, taps_ref, wt_ref, filt_ref, out_ref, buf_ref, ext_ref, res_ref, in_sem, out_sem):
    fetch = [pltpu.make_async_copy(filt_ref.at[b], buf_ref.at[b], in_sem.at[b]) for b in range(BEAMS)]
    send = [pltpu.make_async_copy(res_ref.at[b], out_ref.at[:, b], out_sem.at[b]) for b in range(BEAMS)]
    for copy in fetch:
        copy.start()
    for b in range(BEAMS):
        fetch[b].wait()
        for op in range(4):
            o, p = divmod(op, 2)
            for c in range(N // 128):
                lanes = pl.ds(c * 128, 128)
                slot = (b % 2) * 16 + op * 4 + c
                ext_ref[slot, 0:8, :] = tail_ref[b, op, :, lanes].astype(f32)
                ext_ref[slot, 8:16, :] = halo_ref[b, op, :, lanes].astype(f32)
                acc = taps_ref[0:1, lanes] * ext_ref[slot, 0:8, :]
                for tap in range(1, TAPS):
                    acc = acc + taps_ref[tap : tap + 1, lanes] * ext_ref[slot, tap : tap + 8, :]
                buf_ref[b, (o + 1) * BLK - 8 : (o + 1) * BLK, p * N + c * 128 : p * N + (c + 1) * 128] = acc.astype(bf16)
        for h in range(2):
            half = slice(h * GRP // 2, (h + 1) * GRP // 2)
            res = lax.dot_general(
                wt_ref[half].reshape(256, 2 * N),
                buf_ref[b],
                (((1,), (1,)), ((), ())),
                preferred_element_type=f32,
            )
            res_ref[b, half] = (res * (N ** -0.5)).astype(bf16).reshape(GRP // 2, 32, 256)
        send[b].start()
    for copy in send:
        copy.wait()


def coarse(tail, halo, small, wt, filt):
    whole = lambda shape: pl.BlockSpec(shape, lambda b: (0,) * len(shape))
    return pl.pallas_call(
        coarse_kernel,
        grid=(1,),
        in_specs=[
            whole((BEAMS, 4, 8, N)),
            whole((BEAMS, 4, 8, N)),
            whole((8, N)),
            whole((GRP, 32, 2 * N)),
            pl.BlockSpec(memory_space=pltpu.HBM),
        ],
        out_specs=pl.BlockSpec(memory_space=pltpu.HBM),
        out_shape=jax.ShapeDtypeStruct((GRP, BEAMS, 32, 256), bf16),
        scratch_shapes=[
            pltpu.VMEM((BEAMS, 256, 2 * N), bf16),
            pltpu.VMEM((32, 16, 128), f32),
            pltpu.VMEM((BEAMS, GRP, 32, 256), bf16),
            pltpu.SemaphoreType.DMA((BEAMS,)),
            pltpu.SemaphoreType.DMA((BEAMS,)),
        ],
        compiler_params=pltpu.CompilerParams(vmem_limit_bytes=46 << 20),
        name="coarse",
    )(tail, halo, small, wt, filt)


def fine_kernel(rate_ref, x_ref, first_ref, second_hbm, perm_ref, out_ref, second_ref, lhs_ref, mix_ref, pow_ref, pow2_ref, sem):
    load = pltpu.make_async_copy(second_hbm, second_ref, sem)
    load.start()

    def beam(b, carry):
        rows = pl.ds(pl.multiple_of(b * 16, 16), 16)
        x = x_ref[:, b].reshape(512, 256)
        for h in range(2):
            y = jnp.dot(first_ref[h * 256 : (h + 1) * 256], x, preferred_element_type=f32).astype(bf16)
            for f in range(8):
                for q in range(2):
                    part = y[(2 * f + q) * 16 : (2 * f + q + 1) * 16]
                    for o in range(2):
                        lhs_ref[8 * h + f, o, rows, q * BLK : (q + 1) * BLK] = part[:, o * BLK : (o + 1) * BLK]
        return carry

    lax.fori_loop(0, BEAMS, beam, 0, unroll=4)
    load.wait()
    for f in range(GRP):
        total = None
        for o in range(2):
            z = jnp.dot(lhs_ref[f, o], second_ref[f], preferred_element_type=f32)
            part = z[:, 0:BLK] * z[:, 0:BLK] + z[:, BLK : 2 * BLK] * z[:, BLK : 2 * BLK]
            total = part if total is None else total + part
        pow2_ref[f] = total * (1.0 / 8192.0)
    lane = lax.broadcasted_iota(jnp.int32, (16, 128), 1)

    def mix(b, carry):
        rows = pl.ds(pl.multiple_of(b * 16, 16), 16)
        for h in range(2):
            v = [pow2_ref[8 * h + i, rows, :] for i in range(8)]
            for bit in (1, 2, 4):
                odd = (lane // (16 * bit)) % 2 == 1
                v = [jnp.where(odd, v[(m + bit) % 8], v[m]) for m in range(8)]
            for m in range(8):
                mix_ref[(8 - m) % 8, rows, h * 128 : (h + 1) * 128] = v[m].astype(bf16)
        return carry

    lax.fori_loop(0, BEAMS, mix, 0, unroll=2)
    zero = jnp.zeros((128, 128), f32)
    for e in (0, 1, 18, 19, 20):
        pow_ref[e] = zero
    for m in range(8):
        spots = [h * BLK + 16 * ((p - m) % 8) for h in range(2) for p in range(8)]
        turned = jnp.concatenate([perm_ref[r : r + 16] for r in spots], axis=0)
        q = jnp.dot(mix_ref[m], turned, preferred_element_type=f32)
        for h in range(2):
            for b in range(BEAMS):
                tile = q[b * 16 : (b + 1) * 16, h * 128 : (h + 1) * 128]
                pow_ref[2 + 2 * m + h, pl.ds(b, 16, stride=8), :] = tile
    low_lane = lax.broadcasted_iota(jnp.int32, (8, 128), 1)
    step = lax.axis_index(("x", "zh"))
    own = lax.axis_index(("zl", "y", "core")) * 16

    def shift(pair, carry):
        both = []
        for e in range(2):
            ch = 2 * pair + e
            start = 256 + rate_ref[0, own + ch] * step
            base = lax.shift_right_logical(start, 7)
            off = start & 127
            rows = pl.ds(pl.multiple_of(ch * 8, 8), 8)
            last = low_lane >= off
            r = [pow_ref[base + k, rows, :] for k in range(19)]
            both.append([pltpu.roll(jnp.where(last, r[k], r[k + 1]), (128 - off) & 127, 1) for k in range(18)])
        rows = pl.ds(pl.multiple_of(pair * 16, 16), 16)
        tiles = [jnp.concatenate([both[0][k], both[1][k]], axis=0).astype(bf16) for k in range(18)]
        for x in range(4):
            for w in range(WIN // 128):
                out_ref[x, rows, w * 128 : (w + 1) * 128] = tiles[4 * x + w]
        return carry

    lax.fori_loop(0, 8, shift, 0, unroll=2)


def fine(rates, x, first, second, perm):
    vmem = pl.BlockSpec(memory_space=pltpu.VMEM)
    return pl.pallas_call(
        fine_kernel,
        in_specs=[
            pl.BlockSpec(memory_space=pltpu.SMEM),
            vmem,
            vmem,
            pl.BlockSpec(memory_space=pltpu.HBM),
            vmem,
        ],
        out_specs=vmem,
        out_shape=jax.ShapeDtypeStruct((4, 128, WIN), bf16),
        scratch_shapes=[
            pltpu.VMEM((GRP, 256, 256), bf16),
            pltpu.VMEM((GRP, 2, 128, 256), bf16),
            pltpu.VMEM((8, 128, 256), bf16),
            pltpu.VMEM((21, 128, 128), f32),
            pltpu.VMEM((GRP, 128, 128), f32),
            pltpu.SemaphoreType.DMA,
        ],
        compiler_params=pltpu.CompilerParams(vmem_limit_bytes=50 << 20),
        name="fine",
    )(rates, x, first, second, perm)


def drift_kernel(x_ref, out_ref, sum_ref):
    lane = lax.broadcasted_iota(jnp.int16, (16, 128), 1)

    def body(pair, carry):
        rows = pl.ds(pl.multiple_of(pair * 16, 16), 16)
        for j in range(NDRIFT):
            acc = None
            for t in range(STEPS):
                base, off = divmod(j * t, 128)
                r = [x_ref[t, rows, (base + k) * 128 : (base + k + 1) * 128] for k in range(5 if off else 4)]
                if off:
                    keep = lane >= jnp.int16(off)
                    r = [pltpu.roll(jnp.where(keep, r[k], r[k + 1]), 128 - off, 1) for k in range(4)]
                w = [r[k].astype(f32) for k in range(4)]
                acc = w if acc is None else [acc[k] + w[k] for k in range(4)]
            for k in range(4):
                done = acc[k] * (1.0 / STEPS)
                for e in range(2):
                    at = (2 * pair + e) * NDRIFT + j
                    sum_ref[k, pl.ds(at, 8, stride=64), :] = done[8 * e : 8 * e + 8]
        return carry

    lax.fori_loop(0, 2, body, 0)
    for k in range(4):
        out_ref[:, k * 128 : (k + 1) * 128] = sum_ref[k]


def drift(x):
    return pl.pallas_call(
        drift_kernel,
        in_specs=[pl.BlockSpec(memory_space=pltpu.VMEM)],
        out_specs=pl.BlockSpec(memory_space=pltpu.VMEM),
        out_shape=jax.ShapeDtypeStruct((BEAMS * 64, BINS), f32),
        scratch_shapes=[
            pltpu.VMEM((4, BEAMS * 64, 128), f32),
        ],
        compiler_params=pltpu.CompilerParams(vmem_limit_bytes=50 << 20),
        name="drift",
    )(x)


def shards(voltages, taps, busy_mask, drift_low):
    axes = ("x", "zh", "zl", "y", "core")
    devices = lax.axis_size(axes)
    head = lax.slice_in_dim(voltages, 0, 8, axis=2)
    halo = lax.ppermute(head, axes, [(i + 1, i) for i in range(devices - 1)])
    first, second, perm = fine_tables()
    row = lax.broadcasted_iota(jnp.int32, (8, N), 0)
    extra = jnp.where(row == TAPS, busy_mask[None, :], drift_low[None, :]).astype(f32)
    small = jnp.where(row < TAPS, jnp.pad(taps, ((0, 4), (0, 0))), extra)
    wt, rates, tail, filt = front(small, voltages)
    blocks = coarse(tail, halo, small, wt, filt)
    times = lax.all_to_all(blocks, ("zl", "y", "core"), split_axis=0, concat_axis=0, tiled=True)
    powers = fine(rates, times, jnp.asarray(first), jnp.asarray(second), jnp.asarray(perm))
    wins = lax.all_to_all(powers.reshape(16, 32, WIN), ("x", "zh"), split_axis=0, concat_axis=0, tiled=True)
    out = drift(wins)
    return out.reshape(BEAMS, 4, NDRIFT, BINS)


def solution(mesh):
    fold = Mesh(mesh.devices.reshape(4, 4, 2, 4, 2), ("x", "zh", "zl", "y", "core"))
    chan = ("zh", "zl", "y", "core")
    in_specs = (P(None, None, ("x",) + chan, None), P(), P(), P())
    out_specs = P(None, chan, None, "x")
    return jax.shard_map(shards, mesh=fold, in_specs=in_specs, out_specs=out_specs, check_vma=False)
```

```python
import math

import jax
import jax.numpy as jnp
import numpy as np
from jax import lax
from jax.experimental import pallas as pl
from jax.experimental.pallas import tpu as pltpu
from jax.sharding import Mesh, PartitionSpec as P

TAPS = 4
NDRIFT = 16
N = 512
FINE = 2048
BEAMS = 8
STEPS = 16
BLK = 128
GRP = 16
WIN = 768
BINS = 512
f32 = jnp.float32
bf16 = jnp.bfloat16


def np_bf16(a):
    return np.asarray(a, np.float32).astype(jnp.bfloat16)


def fine_tables():
    k = np.arange(GRP)
    ang = (k[:, None] * k[None, :]) % GRP * (2.0 * math.pi / GRP)
    c, sn = np.cos(ang), np.sin(ang)
    eye = np.eye(16)
    first = np.zeros((GRP, 2, 16, GRP, 2, 16))
    for q, p, val in ((0, 0, c), (0, 1, sn), (1, 0, -sn), (1, 1, c)):
        first[:, q, :, :, p, :] = val[:, None, :, None] * eye[None, :, None, :]
    f1 = np.arange(GRP)
    lane = np.arange(BLK)
    block = (lane[None, :] // 16 - f1[:, None]) % 8
    f2 = block * 16 + lane[None, :] % 16
    j = np.arange(BLK)
    ang = (j[None, :, None] * (f1[:, None] + 16 * f2)[:, None, :]) % FINE * (2.0 * math.pi / FINE)
    c, sn = np.cos(ang), np.sin(ang)
    second = np.concatenate([np.concatenate([c, -sn], 2), np.concatenate([sn, c], 2)], 1)
    perm = np.zeros((256, 256))
    for h in range(2):
        perm[h * 128 + lane, 8 * h + lane // 16 + 16 * (lane % 16)] = 1.0
    return np_bf16(first.reshape(512, 512)), np_bf16(second), np_bf16(perm)


def cos_sin(phase):
    quarter = lax.shift_right_arithmetic(phase + 64, 7)
    x = (phase - quarter * 128).astype(f32) * (2.0 * math.pi / N)
    y = x * x
    c = 1.0 + y * (-0.5 + y * (1.0 / 24 + y * (-1.0 / 720 + y * (1.0 / 40320))))
    s = x * (1.0 + y * (-1.0 / 6 + y * (1.0 / 120 + y * (-1.0 / 5040 + y * (1.0 / 362880)))))
    swap = (quarter & 1) == 1
    cos = jnp.where(swap, s, c)
    sin = jnp.where(swap, c, s)
    cos = jnp.where(((quarter + 1) & 2) == 2, -cos, cos)
    sin = jnp.where((quarter & 2) == 2, -sin, sin)
    return cos, sin


def write_tables(small_ref, wt_ref, rate_ref, hit_ref):
    busy = small_ref[TAPS : TAPS + 1]
    row = lax.broadcasted_iota(jnp.int32, (N, N), 0)
    col = lax.broadcasted_iota(jnp.int32, (N, N), 1)
    upper = (row < col).astype(f32).astype(bf16)
    mask = jnp.broadcast_to(busy, (8, N))
    before = jnp.dot(mask.astype(bf16), upper, preferred_element_type=f32)[0:1].astype(jnp.int32)
    before = jnp.where(busy > 0.5, before, -1)
    for r0 in range(0, 256, 16):
        rp = r0 + lax.broadcasted_iota(jnp.int32, (16, N), 0)
        pos = lax.broadcasted_iota(jnp.int32, (16, N), 1)
        hit = before == (rp // 4) % 4 * 64 + rp // 16 * 4 + rp % 4
        hit_ref[r0 : r0 + 16] = hit.astype(f32).astype(bf16)
        chan = jnp.sum(jnp.where(hit, pos, 0), axis=1, keepdims=True)
        cos, sin = cos_sin((chan * pos[:, 0:BLK]) & (N - 1))
        for c in range(N // BLK):
            turns = (chan * c) & 3
            odd = (turns & 1) == 1
            cos_sign = jnp.where((turns == 1) | (turns == 2), -1.0, 1.0)
            sin_sign = jnp.where(turns >= 2, -1.0, 1.0)
            cc = jnp.where(odd, sin, cos) * cos_sign
            ss = jnp.where(odd, cos, sin) * sin_sign
            lanes = slice(c * BLK, (c + 1) * BLK)
            high = slice(N + c * BLK, N + (c + 1) * BLK)
            wt_ref[r0 // 16, 0:16, lanes] = cc.astype(bf16)
            wt_ref[r0 // 16, 0:16, high] = ss.astype(bf16)
            wt_ref[r0 // 16, 16:32, lanes] = (-ss).astype(bf16)
            wt_ref[r0 // 16, 16:32, high] = cc.astype(bf16)
    low = jnp.broadcast_to(small_ref[TAPS + 1 : TAPS + 2], (8, N)).astype(bf16)
    rate = lax.dot_general(low, hit_ref[...], (((1,), (1,)), ((), ())), preferred_element_type=f32)
    rate_ref[...] = rate[0:1].astype(jnp.int32)


def front_kernel(small_ref, v_ref, wt_ref, rate_ref, tail_ref, filt_ref, buf_ref, ext_ref, hit_ref, sem):
    def fetch(b):
        return pltpu.make_async_copy(v_ref.at[b], buf_ref.at[b], sem.at[b])

    for b in range(BEAMS):
        fetch(b).start()
    write_tables(small_ref, wt_ref, rate_ref, hit_ref)
    for e in range(2 * N // 128):
        ext_ref[e, BLK : BLK + 8, :] = jnp.zeros((8, 128), f32)

    def beam(b, carry):
        fetch(b).wait()
        tail_ref[b] = buf_ref[b, :, BLK - 8 : BLK, :]

        def body(o, inner):
            row = pl.multiple_of(o * BLK, BLK)
            for p in range(2):
                for c in range(N // 128):
                    e = p * (N // 128) + c
                    lanes = pl.ds(c * 128, 128)
                    main = buf_ref[b, 2 * o + p, :, lanes].astype(f32)
                    ext_ref[e, 0:BLK, :] = main
                    acc = small_ref[0:1, lanes] * main
                    for tap in range(1, TAPS):
                        acc = acc + small_ref[tap : tap + 1, lanes] * ext_ref[e, tap : tap + BLK, :]
                    filt_ref[b, pl.ds(row, BLK), e * 128 : (e + 1) * 128] = acc.astype(bf16)
            return inner

        return lax.fori_loop(0, 2, body, carry)

    lax.fori_loop(0, BEAMS, beam, 0)


def front(small, volt):
    vmem = pl.BlockSpec(memory_space=pltpu.VMEM)
    return pl.pallas_call(
        front_kernel,
        in_specs=[vmem, pl.BlockSpec(memory_space=pltpu.HBM)],
        out_specs=(vmem,) * 4,
        out_shape=(
            jax.ShapeDtypeStruct((GRP, 32, 2 * N), bf16),
            jax.ShapeDtypeStruct((1, 256), jnp.int32),
            jax.ShapeDtypeStruct((BEAMS, 4, 8, N), bf16),
            jax.ShapeDtypeStruct((BEAMS, 256, 2 * N), bf16),
        ),
        scratch_shapes=[
            pltpu.VMEM((BEAMS, 4, BLK, N), bf16),
            pltpu.VMEM((2 * N // 128, BLK + 8, 128), f32),
            pltpu.VMEM((256, N), bf16),
            pltpu.SemaphoreType.DMA((BEAMS,)),
        ],
        compiler_params=pltpu.CompilerParams(vmem_limit_bytes=46 << 20),
        name="front",
    )(small, volt)


def coarse_kernel(tail_ref, halo_ref, small_ref, wt_ref, filt_ref, out_ref, buf_ref, ext_ref):
    for b in range(BEAMS):
        for op in range(4):
            o, p = divmod(op, 2)
            for c in range(N // 128):
                lanes = pl.ds(c * 128, 128)
                slot = (b % 2) * 16 + op * 4 + c
                ext_ref[slot, 0:8, :] = tail_ref[b, op, :, lanes].astype(f32)
                ext_ref[slot, 8:16, :] = halo_ref[b, op, :, lanes].astype(f32)
                acc = small_ref[0:1, lanes] * ext_ref[slot, 0:8, :]
                for tap in range(1, TAPS):
                    acc = acc + small_ref[tap : tap + 1, lanes] * ext_ref[slot, tap : tap + 8, :]
                buf_ref[b, (o + 1) * BLK - 8 : (o + 1) * BLK, p * N + c * 128 : p * N + (c + 1) * 128] = acc.astype(bf16)
        for h in range(2):
            half = slice(h * GRP // 2, (h + 1) * GRP // 2)
            res = lax.dot_general(
                wt_ref[half].reshape(256, 2 * N),
                buf_ref[b],
                (((1,), (1,)), ((), ())),
                preferred_element_type=f32,
            )
            out_ref[half, b] = (res * (N ** -0.5)).astype(bf16).reshape(GRP // 2, 32, 256)


def coarse(tail, halo, small, wt, filt):
    vmem = pl.BlockSpec(memory_space=pltpu.VMEM)
    return pl.pallas_call(
        coarse_kernel,
        in_specs=[vmem] * 5,
        out_specs=(vmem, vmem),
        out_shape=(
            jax.ShapeDtypeStruct((GRP, BEAMS, 32, 256), bf16),
            jax.ShapeDtypeStruct((BEAMS, 256, 2 * N), bf16),
        ),
        input_output_aliases={4: 1},
        scratch_shapes=[pltpu.VMEM((32, 16, 128), f32)],
        compiler_params=pltpu.CompilerParams(vmem_limit_bytes=46 << 20),
        name="coarse",
    )(tail, halo, small, wt, filt)


def fine_kernel(rate_ref, x_ref, first_ref, second_hbm, perm_ref, out_ref, second_ref, lhs_ref, mix_ref, pow_ref, pow2_ref, sem):
    load = pltpu.make_async_copy(second_hbm, second_ref, sem)
    load.start()

    def beam(b, carry):
        rows = pl.ds(pl.multiple_of(b * 16, 16), 16)
        x = x_ref[:, b].reshape(512, 256)
        for h in range(2):
            y = jnp.dot(first_ref[h * 256 : (h + 1) * 256], x, preferred_element_type=f32).astype(bf16)
            for f in range(8):
                for q in range(2):
                    part = y[(2 * f + q) * 16 : (2 * f + q + 1) * 16]
                    for o in range(2):
                        lhs_ref[8 * h + f, o, rows, q * BLK : (q + 1) * BLK] = part[:, o * BLK : (o + 1) * BLK]
        return carry

    lax.fori_loop(0, BEAMS, beam, 0, unroll=4)
    load.wait()
    for f in range(GRP):
        total = None
        for o in range(2):
            z = jnp.dot(lhs_ref[f, o], second_ref[f], preferred_element_type=f32)
            part = z[:, 0:BLK] * z[:, 0:BLK] + z[:, BLK : 2 * BLK] * z[:, BLK : 2 * BLK]
            total = part if total is None else total + part
        pow2_ref[f] = total * (1.0 / 8192.0)
    lane = lax.broadcasted_iota(jnp.int32, (16, 128), 1)

    def mix(b, carry):
        rows = pl.ds(pl.multiple_of(b * 16, 16), 16)
        for h in range(2):
            v = [pow2_ref[8 * h + i, rows, :] for i in range(8)]
            for bit in (1, 2, 4):
                odd = (lane // (16 * bit)) % 2 == 1
                v = [jnp.where(odd, v[(m + bit) % 8], v[m]) for m in range(8)]
            for m in range(8):
                mix_ref[(8 - m) % 8, rows, h * 128 : (h + 1) * 128] = v[m].astype(bf16)
        return carry

    lax.fori_loop(0, BEAMS, mix, 0, unroll=2)
    zero = jnp.zeros((128, 128), f32)
    for e in (0, 1, 18, 19, 20):
        pow_ref[e] = zero
    for m in range(8):
        spots = [h * BLK + 16 * ((p - m) % 8) for h in range(2) for p in range(8)]
        turned = jnp.concatenate([perm_ref[r : r + 16] for r in spots], axis=0)
        q = jnp.dot(mix_ref[m], turned, preferred_element_type=f32)
        for h in range(2):
            for b in range(BEAMS):
                tile = q[b * 16 : (b + 1) * 16, h * 128 : (h + 1) * 128]
                pow_ref[2 + 2 * m + h, pl.ds(b, 16, stride=8), :] = tile
    low_lane = lax.broadcasted_iota(jnp.int32, (8, 128), 1)
    step = lax.axis_index(("x", "zh"))
    own = lax.axis_index(("zl", "y", "core")) * 16

    def shift(pair, carry):
        both = []
        for e in range(2):
            ch = 2 * pair + e
            start = 256 + rate_ref[0, own + ch] * step
            base = lax.shift_right_logical(start, 7)
            off = start & 127
            rows = pl.ds(pl.multiple_of(ch * 8, 8), 8)
            last = low_lane >= off
            r = [pow_ref[base + k, rows, :] for k in range(19)]
            both.append([pltpu.roll(jnp.where(last, r[k], r[k + 1]), (128 - off) & 127, 1) for k in range(18)])
        rows = pl.ds(pl.multiple_of(pair * 16, 16), 16)
        tiles = [jnp.concatenate([both[0][k], both[1][k]], axis=0).astype(bf16) for k in range(18)]
        for x in range(4):
            for w in range(WIN // 128):
                out_ref[x, rows, w * 128 : (w + 1) * 128] = tiles[4 * x + w]
        return carry

    lax.fori_loop(0, 8, shift, 0, unroll=2)


def fine(rates, x, first, second, perm):
    vmem = pl.BlockSpec(memory_space=pltpu.VMEM)
    return pl.pallas_call(
        fine_kernel,
        in_specs=[
            pl.BlockSpec(memory_space=pltpu.SMEM),
            vmem,
            vmem,
            pl.BlockSpec(memory_space=pltpu.HBM),
            vmem,
        ],
        out_specs=vmem,
        out_shape=jax.ShapeDtypeStruct((4, 128, WIN), bf16),
        scratch_shapes=[
            pltpu.VMEM((GRP, 256, 256), bf16),
            pltpu.VMEM((GRP, 2, 128, 256), bf16),
            pltpu.VMEM((8, 128, 256), bf16),
            pltpu.VMEM((21, 128, 128), f32),
            pltpu.VMEM((GRP, 128, 128), f32),
            pltpu.SemaphoreType.DMA,
        ],
        compiler_params=pltpu.CompilerParams(vmem_limit_bytes=50 << 20),
        name="fine",
    )(rates, x, first, second, perm)


def drift_kernel(x_ref, out_ref, sum_ref):
    lane = lax.broadcasted_iota(jnp.int16, (16, 128), 1)

    def body(pair, carry):
        rows = pl.ds(pl.multiple_of(pair * 16, 16), 16)
        for j in range(NDRIFT):
            acc = None
            for t in range(STEPS):
                base, off = divmod(j * t, 128)
                r = [x_ref[t, rows, (base + k) * 128 : (base + k + 1) * 128] for k in range(5 if off else 4)]
                if off:
                    keep = lane >= jnp.int16(off)
                    r = [pltpu.roll(jnp.where(keep, r[k], r[k + 1]), 128 - off, 1) for k in range(4)]
                w = [r[k].astype(f32) for k in range(4)]
                acc = w if acc is None else [acc[k] + w[k] for k in range(4)]
            for k in range(4):
                done = acc[k] * (1.0 / STEPS)
                for e in range(2):
                    at = (2 * pair + e) * NDRIFT + j
                    sum_ref[k, pl.ds(at, 8, stride=64), :] = done[8 * e : 8 * e + 8]
        return carry

    lax.fori_loop(0, 2, body, 0)
    for k in range(4):
        out_ref[:, k * 128 : (k + 1) * 128] = sum_ref[k]


def drift(x):
    return pl.pallas_call(
        drift_kernel,
        in_specs=[pl.BlockSpec(memory_space=pltpu.VMEM)],
        out_specs=pl.BlockSpec(memory_space=pltpu.VMEM),
        out_shape=jax.ShapeDtypeStruct((BEAMS * 64, BINS), f32),
        scratch_shapes=[
            pltpu.VMEM((4, BEAMS * 64, 128), f32),
        ],
        compiler_params=pltpu.CompilerParams(vmem_limit_bytes=50 << 20),
        name="drift",
    )(x)


def shards(voltages, taps, busy_mask, drift_low):
    axes = ("x", "zh", "zl", "y", "core")
    devices = lax.axis_size(axes)
    head = lax.slice_in_dim(voltages, 0, 8, axis=2)
    halo = lax.ppermute(head, axes, [(i + 1, i) for i in range(devices - 1)])
    first, second, perm = fine_tables()
    row = lax.broadcasted_iota(jnp.int32, (8, N), 0)
    extra = jnp.where(row == TAPS, busy_mask[None, :], drift_low[None, :]).astype(f32)
    small = jnp.where(row < TAPS, jnp.pad(taps, ((0, 4), (0, 0))), extra)
    wt, rates, tail, filt = front(small, voltages)
    blocks, _ = coarse(tail, halo, small, wt, filt)
    times = lax.all_to_all(blocks, ("zl", "y", "core"), split_axis=0, concat_axis=0, tiled=True)
    powers = fine(rates, times, jnp.asarray(first), jnp.asarray(second), jnp.asarray(perm))
    wins = lax.all_to_all(powers.reshape(16, 32, WIN), ("x", "zh"), split_axis=0, concat_axis=0, tiled=True)
    out = drift(wins)
    return out.reshape(BEAMS, 4, NDRIFT, BINS)


def solution(mesh):
    fold = Mesh(mesh.devices.reshape(4, 4, 2, 4, 2), ("x", "zh", "zl", "y", "core"))
    chan = ("zh", "zl", "y", "core")
    in_specs = (P(None, None, ("x",) + chan, None), P(), P(), P())
    out_specs = P(None, chan, None, "x")
    return jax.shard_map(shards, mesh=fold, in_specs=in_specs, out_specs=out_specs, check_vma=False)
```

```python
import math

import jax
import jax.numpy as jnp
import numpy as np
from jax import lax
from jax.experimental import pallas as pl
from jax.experimental.pallas import tpu as pltpu
from jax.sharding import Mesh, PartitionSpec as P

TAPS = 4
HALO = 4
NDRIFT = 16
N = 512
FINE = 2048
BEAMS = 8
STEPS = 16
BLK = 128
GRP = 16
WIN = 768
BINS = 512
f32 = jnp.float32
bf16 = jnp.bfloat16


def np_bf16(a):
    return np.asarray(a, np.float32).astype(jnp.bfloat16)


def fine_tables():
    k = np.arange(GRP)
    ang = (k[:, None] * k[None, :]) % GRP * (2.0 * math.pi / GRP)
    c, sn = np.cos(ang), np.sin(ang)
    eye = np.eye(16)
    first = np.zeros((GRP, 2, 16, GRP, 2, 16))
    for q, p, val in ((0, 0, c), (0, 1, sn), (1, 0, -sn), (1, 1, c)):
        first[:, q, :, :, p, :] = val[:, None, :, None] * eye[None, :, None, :]
    f1 = np.arange(GRP)
    lane = np.arange(BLK)
    block = (lane[None, :] // 16 - f1[:, None]) % 8
    f2 = block * 16 + lane[None, :] % 16
    j = np.arange(BLK)
    ang = (j[None, :, None] * (f1[:, None] + 16 * f2)[:, None, :]) % FINE * (2.0 * math.pi / FINE)
    c, sn = np.cos(ang), np.sin(ang)
    second = np.concatenate([np.concatenate([c, -sn], 2), np.concatenate([sn, c], 2)], 1)
    perm = np.zeros((256, 256))
    for h in range(2):
        perm[h * 128 + lane, 8 * h + lane // 16 + 16 * (lane % 16)] = 1.0
    return np_bf16(first.reshape(512, 512)), np_bf16(second), np_bf16(perm)


def cos_sin(phase):
    quarter = lax.shift_right_arithmetic(phase + 64, 7)
    x = (phase - quarter * 128).astype(f32) * (2.0 * math.pi / N)
    y = x * x
    c = 1.0 + y * (-0.5 + y * (1.0 / 24 + y * (-1.0 / 720 + y * (1.0 / 40320))))
    s = x * (1.0 + y * (-1.0 / 6 + y * (1.0 / 120 + y * (-1.0 / 5040 + y * (1.0 / 362880)))))
    swap = (quarter & 1) == 1
    cos = jnp.where(swap, s, c)
    sin = jnp.where(swap, c, s)
    cos = jnp.where(((quarter + 1) & 2) == 2, -cos, cos)
    sin = jnp.where((quarter & 2) == 2, -sin, sin)
    return cos, sin


def write_tables(small_ref, wt_ref, rate_ref, hit_ref):
    busy = small_ref[TAPS : TAPS + 1]
    row = lax.broadcasted_iota(jnp.int32, (N, N), 0)
    col = lax.broadcasted_iota(jnp.int32, (N, N), 1)
    upper = (row < col).astype(f32).astype(bf16)
    mask = jnp.broadcast_to(busy, (8, N))
    before = jnp.dot(mask.astype(bf16), upper, preferred_element_type=f32)[0:1].astype(jnp.int32)
    before = jnp.where(busy > 0.5, before, -1)
    for r0 in range(0, 256, 16):
        rp = r0 + lax.broadcasted_iota(jnp.int32, (16, N), 0)
        pos = lax.broadcasted_iota(jnp.int32, (16, N), 1)
        hit = before == (rp // 4) % 4 * 64 + rp // 16 * 4 + rp % 4
        hit_ref[r0 : r0 + 16] = hit.astype(f32).astype(bf16)
        chan = jnp.sum(jnp.where(hit, pos, 0), axis=1, keepdims=True)
        cos, sin = cos_sin((chan * pos[:, 0:BLK]) & (N - 1))
        for c in range(N // BLK):
            turns = (chan * c) & 3
            odd = (turns & 1) == 1
            cos_sign = jnp.where((turns == 1) | (turns == 2), -1.0, 1.0)
            sin_sign = jnp.where(turns >= 2, -1.0, 1.0)
            cc = jnp.where(odd, sin, cos) * cos_sign
            ss = jnp.where(odd, cos, sin) * sin_sign
            lanes = slice(c * BLK, (c + 1) * BLK)
            high = slice(N + c * BLK, N + (c + 1) * BLK)
            wt_ref[r0 // 16, 0:16, lanes] = cc.astype(bf16)
            wt_ref[r0 // 16, 0:16, high] = ss.astype(bf16)
            wt_ref[r0 // 16, 16:32, lanes] = (-ss).astype(bf16)
            wt_ref[r0 // 16, 16:32, high] = cc.astype(bf16)
    low = jnp.broadcast_to(small_ref[TAPS + 1 : TAPS + 2], (8, N)).astype(bf16)
    rate = lax.dot_general(low, hit_ref[...], (((1,), (1,)), ((), ())), preferred_element_type=f32)
    rate_ref[...] = rate[0:1].astype(jnp.int32)


def front_kernel(small_ref, v_ref, wt_ref, rate_ref, tail_ref, filt_ref, buf_ref, ext_ref, hit_ref, sem):
    def fetch(b):
        return pltpu.make_async_copy(v_ref.at[b], buf_ref.at[b], sem.at[b])

    for b in range(BEAMS):
        fetch(b).start()
    write_tables(small_ref, wt_ref, rate_ref, hit_ref)
    for e in range(2 * N // 128):
        ext_ref[e, BLK : BLK + 8, :] = jnp.zeros((8, 128), f32)

    def beam(b, carry):
        fetch(b).wait()
        tail_ref[b] = buf_ref[b, :, BLK - 8 : BLK, :]

        def body(o, inner):
            row = pl.multiple_of(o * BLK, BLK)
            for p in range(2):
                for c in range(N // 128):
                    e = p * (N // 128) + c
                    lanes = pl.ds(c * 128, 128)
                    main = buf_ref[b, 2 * o + p, :, lanes].astype(f32)
                    ext_ref[e, 0:BLK, :] = main
                    acc = small_ref[0:1, lanes] * main
                    for tap in range(1, TAPS):
                        acc = acc + small_ref[tap : tap + 1, lanes] * ext_ref[e, tap : tap + BLK, :]
                    filt_ref[b, pl.ds(row, BLK), e * 128 : (e + 1) * 128] = acc.astype(bf16)
            return inner

        return lax.fori_loop(0, 2, body, carry)

    lax.fori_loop(0, BEAMS, beam, 0)


def front(small, volt):
    vmem = pl.BlockSpec(memory_space=pltpu.VMEM)
    return pl.pallas_call(
        front_kernel,
        in_specs=[vmem, pl.BlockSpec(memory_space=pltpu.HBM)],
        out_specs=(vmem,) * 4,
        out_shape=(
            jax.ShapeDtypeStruct((GRP, 32, 2 * N), bf16),
            jax.ShapeDtypeStruct((1, 256), jnp.int32),
            jax.ShapeDtypeStruct((BEAMS, 4, 8, N), bf16),
            jax.ShapeDtypeStruct((BEAMS, 256, 2 * N), bf16),
        ),
        scratch_shapes=[
            pltpu.VMEM((BEAMS, 4, BLK, N), bf16),
            pltpu.VMEM((2 * N // 128, BLK + 8, 128), f32),
            pltpu.VMEM((256, N), bf16),
            pltpu.SemaphoreType.DMA((BEAMS,)),
        ],
        compiler_params=pltpu.CompilerParams(vmem_limit_bytes=46 << 20),
        name="front",
    )(small, volt)


def coarse_kernel(tail_ref, halo_ref, small_ref, wt_ref, filt_ref, out_ref, buf_ref, ext_ref):
    for b in range(BEAMS):
        for op in range(4):
            o, p = divmod(op, 2)
            for c in range(N // 128):
                lanes = pl.ds(c * 128, 128)
                slot = (b % 2) * 16 + op * 4 + c
                ext_ref[slot, 0:8, :] = tail_ref[b, op, :, lanes].astype(f32)
                ext_ref[slot, 8 : 8 + HALO, :] = halo_ref[b, op, :, lanes].astype(f32)
                acc = small_ref[0:1, lanes] * ext_ref[slot, 0:8, :]
                for tap in range(1, TAPS):
                    acc = acc + small_ref[tap : tap + 1, lanes] * ext_ref[slot, tap : tap + 8, :]
                buf_ref[b, (o + 1) * BLK - 8 : (o + 1) * BLK, p * N + c * 128 : p * N + (c + 1) * 128] = acc.astype(bf16)
        for h in range(2):
            half = slice(h * GRP // 2, (h + 1) * GRP // 2)
            res = lax.dot_general(
                wt_ref[half].reshape(256, 2 * N),
                buf_ref[b],
                (((1,), (1,)), ((), ())),
                preferred_element_type=f32,
            )
            out_ref[half, b] = (res * (N ** -0.5)).astype(bf16).reshape(GRP // 2, 32, 256)


def coarse(tail, halo, small, wt, filt):
    vmem = pl.BlockSpec(memory_space=pltpu.VMEM)
    return pl.pallas_call(
        coarse_kernel,
        in_specs=[vmem] * 5,
        out_specs=(vmem, vmem),
        out_shape=(
            jax.ShapeDtypeStruct((GRP, BEAMS, 32, 256), bf16),
            jax.ShapeDtypeStruct((BEAMS, 256, 2 * N), bf16),
        ),
        input_output_aliases={4: 1},
        scratch_shapes=[pltpu.VMEM((32, 16, 128), f32)],
        compiler_params=pltpu.CompilerParams(vmem_limit_bytes=46 << 20),
        name="coarse",
    )(tail, halo, small, wt, filt)


def fine_kernel(rate_ref, x_ref, first_ref, second_hbm, perm_ref, out_ref, second_ref, lhs_ref, mix_ref, pow_ref, pow2_ref, sem):
    load = pltpu.make_async_copy(second_hbm, second_ref, sem)
    load.start()

    def beam(b, carry):
        rows = pl.ds(pl.multiple_of(b * 16, 16), 16)
        x = x_ref[:, b].reshape(512, 256)
        for h in range(2):
            y = jnp.dot(first_ref[h * 256 : (h + 1) * 256], x, preferred_element_type=f32).astype(bf16)
            for f in range(8):
                for q in range(2):
                    part = y[(2 * f + q) * 16 : (2 * f + q + 1) * 16]
                    for o in range(2):
                        lhs_ref[8 * h + f, o, rows, q * BLK : (q + 1) * BLK] = part[:, o * BLK : (o + 1) * BLK]
        return carry

    lax.fori_loop(0, BEAMS, beam, 0, unroll=4)
    load.wait()
    for f in range(GRP):
        total = None
        for o in range(2):
            z = jnp.dot(lhs_ref[f, o], second_ref[f], preferred_element_type=f32)
            part = z[:, 0:BLK] * z[:, 0:BLK] + z[:, BLK : 2 * BLK] * z[:, BLK : 2 * BLK]
            total = part if total is None else total + part
        pow2_ref[f] = total * (1.0 / 8192.0)
    lane = lax.broadcasted_iota(jnp.int32, (16, 128), 1)

    def mix(b, carry):
        rows = pl.ds(pl.multiple_of(b * 16, 16), 16)
        for h in range(2):
            v = [pow2_ref[8 * h + i, rows, :] for i in range(8)]
            for bit in (1, 2, 4):
                odd = (lane // (16 * bit)) % 2 == 1
                v = [jnp.where(odd, v[(m + bit) % 8], v[m]) for m in range(8)]
            for m in range(8):
                mix_ref[(8 - m) % 8, rows, h * 128 : (h + 1) * 128] = v[m].astype(bf16)
        return carry

    lax.fori_loop(0, BEAMS, mix, 0, unroll=2)
    zero = jnp.zeros((128, 128), f32)
    for e in (0, 1, 18, 19, 20):
        pow_ref[e] = zero
    for m in range(8):
        spots = [h * BLK + 16 * ((p - m) % 8) for h in range(2) for p in range(8)]
        turned = jnp.concatenate([perm_ref[r : r + 16] for r in spots], axis=0)
        q = jnp.dot(mix_ref[m], turned, preferred_element_type=f32)
        for h in range(2):
            for b in range(BEAMS):
                tile = q[b * 16 : (b + 1) * 16, h * 128 : (h + 1) * 128]
                pow_ref[2 + 2 * m + h, pl.ds(b, 16, stride=8), :] = tile
    low_lane = lax.broadcasted_iota(jnp.int32, (8, 128), 1)
    step = lax.axis_index(("x", "zh"))
    own = lax.axis_index(("zl", "y", "core")) * 16

    def shift(pair, carry):
        both = []
        for e in range(2):
            ch = 2 * pair + e
            start = 256 + rate_ref[0, own + ch] * step
            base = lax.shift_right_logical(start, 7)
            off = start & 127
            rows = pl.ds(pl.multiple_of(ch * 8, 8), 8)
            last = low_lane >= off
            r = [pow_ref[base + k, rows, :] for k in range(19)]
            both.append([pltpu.roll(jnp.where(last, r[k], r[k + 1]), (128 - off) & 127, 1) for k in range(18)])
        rows = pl.ds(pl.multiple_of((pair % 2) * 16, 16), 16)
        tiles = [jnp.concatenate([both[0][k], both[1][k]], axis=0).astype(bf16) for k in range(18)]
        for x in range(4):
            for w in range(WIN // 128):
                out_ref[pair // 2, x, rows, w * 128 : (w + 1) * 128] = tiles[4 * x + w]
        return carry

    lax.fori_loop(0, 8, shift, 0, unroll=2)


def fine(rates, x, first, second, perm):
    vmem = pl.BlockSpec(memory_space=pltpu.VMEM)
    return pl.pallas_call(
        fine_kernel,
        in_specs=[
            pl.BlockSpec(memory_space=pltpu.SMEM),
            vmem,
            vmem,
            pl.BlockSpec(memory_space=pltpu.HBM),
            vmem,
        ],
        out_specs=vmem,
        out_shape=jax.ShapeDtypeStruct((4, 4, 32, WIN), bf16),
        scratch_shapes=[
            pltpu.VMEM((GRP, 256, 256), bf16),
            pltpu.VMEM((GRP, 2, 128, 256), bf16),
            pltpu.VMEM((8, 128, 256), bf16),
            pltpu.VMEM((21, 128, 128), f32),
            pltpu.VMEM((GRP, 128, 128), f32),
            pltpu.SemaphoreType.DMA,
        ],
        compiler_params=pltpu.CompilerParams(vmem_limit_bytes=50 << 20),
        name="fine",
    )(rates, x, first, second, perm)


def drift_kernel(x_ref, out_ref, sum_ref, stage_ref, sem):
    lane = lax.broadcasted_iota(jnp.int16, (16, 128), 1)

    def send(b, pair):
        part = pl.ds(pl.multiple_of(b * 64 + pair * 32, 32), 32)
        return pltpu.make_async_copy(stage_ref.at[part], out_ref.at[part], sem.at[pair, b])

    def body(pair, carry):
        rows = pl.ds(pl.multiple_of(pair * 16, 16), 16)
        for j in range(NDRIFT):
            acc = None
            for t in range(STEPS):
                base, off = divmod(j * t, 128)
                r = [x_ref[t % 4 * 4 + t // 4, rows, (base + k) * 128 : (base + k + 1) * 128] for k in range(5 if off else 4)]
                if off:
                    keep = lane >= jnp.int16(off)
                    r = [pltpu.roll(jnp.where(keep, r[k], r[k + 1]), 128 - off, 1) for k in range(4)]
                w = [r[k].astype(f32) for k in range(4)]
                acc = w if acc is None else [acc[k] + w[k] for k in range(4)]
            for k in range(4):
                done = acc[k] * (1.0 / STEPS)
                for e in range(2):
                    at = (2 * pair + e) * NDRIFT + j
                    sum_ref[k, pl.ds(at, 8, stride=64), :] = done[8 * e : 8 * e + 8]
        for b in range(BEAMS):
            part = pl.ds(pl.multiple_of(b * 64 + pair * 32, 32), 32)
            for k in range(4):
                stage_ref[part, k * 128 : (k + 1) * 128] = sum_ref[k, part, :]
            send(b, pair).start()
        return carry

    lax.fori_loop(0, 2, body, 0)
    for pair in range(2):
        for b in range(BEAMS):
            send(b, pair).wait()


def drift(x):
    return pl.pallas_call(
        drift_kernel,
        in_specs=[pl.BlockSpec(memory_space=pltpu.VMEM)],
        out_specs=pl.BlockSpec(memory_space=pltpu.HBM),
        out_shape=jax.ShapeDtypeStruct((BEAMS * 64, BINS), f32),
        scratch_shapes=[
            pltpu.VMEM((4, BEAMS * 64, 128), f32),
            pltpu.VMEM((BEAMS * 64, BINS), f32),
            pltpu.SemaphoreType.DMA((2, BEAMS)),
        ],
        compiler_params=pltpu.CompilerParams(vmem_limit_bytes=50 << 20),
        name="drift",
    )(x)


def shards(voltages, taps, busy_mask, drift_low):
    axes = ("x", "zh", "zl", "y", "core")
    devices = lax.axis_size(axes)
    head = lax.slice_in_dim(voltages, 0, HALO, axis=2)
    halo = lax.ppermute(head, axes, [(i + 1, i) for i in range(devices - 1)])
    first, second, perm = fine_tables()
    row = lax.broadcasted_iota(jnp.int32, (8, N), 0)
    extra = jnp.where(row == TAPS, busy_mask[None, :], drift_low[None, :]).astype(f32)
    small = jnp.where(row < TAPS, jnp.pad(taps, ((0, 4), (0, 0))), extra)
    wt, rates, tail, filt = front(small, voltages)
    blocks, _ = coarse(tail, halo, small, wt, filt)
    times = lax.all_to_all(blocks, ("zl", "y", "core"), split_axis=0, concat_axis=0, tiled=True)
    powers = fine(rates, times, jnp.asarray(first), jnp.asarray(second), jnp.asarray(perm))
    wins = lax.all_to_all(powers.reshape(16, 32, WIN), ("zh", "x"), split_axis=0, concat_axis=0, tiled=True)
    out = drift(wins)
    return out.reshape(BEAMS, 4, NDRIFT, BINS)


def solution(mesh):
    fold = Mesh(mesh.devices.reshape(4, 4, 2, 4, 2), ("x", "zh", "zl", "y", "core"))
    chan = ("zh", "zl", "y", "core")
    in_specs = (P(None, None, ("x",) + chan, None), P(), P(), P())
    out_specs = P(None, chan, None, "x")
    return jax.shard_map(shards, mesh=fold, in_specs=in_specs, out_specs=out_specs, check_vma=False)
```

```python
import math

import jax
import jax.numpy as jnp
import numpy as np
from jax import lax
from jax.experimental import pallas as pl
from jax.experimental.pallas import tpu as pltpu
from jax.sharding import Mesh, PartitionSpec as P

TAPS = 4
HALO = 4
NDRIFT = 16
N = 512
FINE = 2048
BEAMS = 8
STEPS = 16
BLK = 128
GRP = 16
WIN = 768
BINS = 512
f32 = jnp.float32
bf16 = jnp.bfloat16


def np_bf16(a):
    return np.asarray(a, np.float32).astype(jnp.bfloat16)


def fine_tables():
    k = np.arange(GRP)
    ang = (k[:, None] * k[None, :]) % GRP * (2.0 * math.pi / GRP)
    c, sn = np.cos(ang), np.sin(ang)
    eye = np.eye(16)
    first = np.zeros((GRP, 2, 16, GRP, 2, 16))
    for q, p, val in ((0, 0, c), (0, 1, sn), (1, 0, -sn), (1, 1, c)):
        first[:, q, :, :, p, :] = val[:, None, :, None] * eye[None, :, None, :]
    f1 = np.arange(GRP)
    lane = np.arange(BLK)
    block = (lane[None, :] // 16 - f1[:, None]) % 8
    f2 = block * 16 + lane[None, :] % 16
    j = np.arange(BLK)
    ang = (j[None, :, None] * (f1[:, None] + 16 * f2)[:, None, :]) % FINE * (2.0 * math.pi / FINE)
    c, sn = np.cos(ang), np.sin(ang)
    second = np.concatenate([np.concatenate([c, -sn], 2), np.concatenate([sn, c], 2)], 1)
    perm = np.zeros((256, 256))
    for h in range(2):
        perm[h * 128 + lane, 8 * h + lane // 16 + 16 * (lane % 16)] = 1.0
    return np_bf16(first.reshape(512, 512)), np_bf16(second), np_bf16(perm)


def cos_sin(phase):
    quarter = lax.shift_right_arithmetic(phase + 64, 7)
    x = (phase - quarter * 128).astype(f32) * (2.0 * math.pi / N)
    y = x * x
    c = 1.0 + y * (-0.5 + y * (1.0 / 24 + y * (-1.0 / 720 + y * (1.0 / 40320))))
    s = x * (1.0 + y * (-1.0 / 6 + y * (1.0 / 120 + y * (-1.0 / 5040 + y * (1.0 / 362880)))))
    swap = (quarter & 1) == 1
    cos = jnp.where(swap, s, c)
    sin = jnp.where(swap, c, s)
    cos = jnp.where(((quarter + 1) & 2) == 2, -cos, cos)
    sin = jnp.where((quarter & 2) == 2, -sin, sin)
    return cos, sin


def write_tables(small_ref, wt_ref, rate_ref, hit_ref):
    busy = small_ref[TAPS : TAPS + 1]
    row = lax.broadcasted_iota(jnp.int32, (N, N), 0)
    col = lax.broadcasted_iota(jnp.int32, (N, N), 1)
    upper = (row < col).astype(f32).astype(bf16)
    mask = jnp.broadcast_to(busy, (8, N))
    before = jnp.dot(mask.astype(bf16), upper, preferred_element_type=f32)[0:1].astype(jnp.int32)
    before = jnp.where(busy > 0.5, before, -1)
    for r0 in range(0, 256, 16):
        rp = r0 + lax.broadcasted_iota(jnp.int32, (16, N), 0)
        pos = lax.broadcasted_iota(jnp.int32, (16, N), 1)
        hit = before == (rp // 4) % 4 * 64 + rp // 16 * 4 + rp % 4
        hit_ref[r0 : r0 + 16] = hit.astype(f32).astype(bf16)
        chan = jnp.sum(jnp.where(hit, pos, 0), axis=1, keepdims=True)
        cos, sin = cos_sin((chan * pos[:, 0:BLK]) & (N - 1))
        for c in range(N // BLK):
            turns = (chan * c) & 3
            odd = (turns & 1) == 1
            cos_sign = jnp.where((turns == 1) | (turns == 2), -1.0, 1.0)
            sin_sign = jnp.where(turns >= 2, -1.0, 1.0)
            cc = jnp.where(odd, sin, cos) * cos_sign
            ss = jnp.where(odd, cos, sin) * sin_sign
            lanes = slice(c * BLK, (c + 1) * BLK)
            high = slice(N + c * BLK, N + (c + 1) * BLK)
            wt_ref[r0 // 16, 0:16, lanes] = cc.astype(bf16)
            wt_ref[r0 // 16, 0:16, high] = ss.astype(bf16)
            wt_ref[r0 // 16, 16:32, lanes] = (-ss).astype(bf16)
            wt_ref[r0 // 16, 16:32, high] = cc.astype(bf16)
    low = jnp.broadcast_to(small_ref[TAPS + 1 : TAPS + 2], (8, N)).astype(bf16)
    rate = lax.dot_general(low, hit_ref[...], (((1,), (1,)), ((), ())), preferred_element_type=f32)
    rate_ref[...] = rate[0:1].astype(jnp.int32)


def front_kernel(small_ref, v_ref, wt_ref, rate_ref, tail_ref, filt_ref, buf_ref, ext_ref, hit_ref, sem):
    def fetch(b):
        return pltpu.make_async_copy(v_ref.at[b], buf_ref.at[b], sem.at[b])

    for b in range(BEAMS):
        fetch(b).start()
    write_tables(small_ref, wt_ref, rate_ref, hit_ref)
    for e in range(2 * N // 128):
        ext_ref[e, BLK : BLK + 8, :] = jnp.zeros((8, 128), f32)

    def beam(b, carry):
        fetch(b).wait()
        tail_ref[b] = buf_ref[b, :, BLK - 8 : BLK, :]

        def body(o, inner):
            row = pl.multiple_of(o * BLK, BLK)
            for p in range(2):
                for c in range(N // 128):
                    e = p * (N // 128) + c
                    lanes = pl.ds(c * 128, 128)
                    main = buf_ref[b, 2 * o + p, :, lanes].astype(f32)
                    ext_ref[e, 0:BLK, :] = main
                    acc = small_ref[0:1, lanes] * main
                    for tap in range(1, TAPS):
                        acc = acc + small_ref[tap : tap + 1, lanes] * ext_ref[e, tap : tap + BLK, :]
                    filt_ref[b, pl.ds(row, BLK), e * 128 : (e + 1) * 128] = acc.astype(bf16)
            return inner

        return lax.fori_loop(0, 2, body, carry, unroll=2)

    lax.fori_loop(0, BEAMS, beam, 0)


def front(small, volt):
    vmem = pl.BlockSpec(memory_space=pltpu.VMEM)
    return pl.pallas_call(
        front_kernel,
        in_specs=[vmem, pl.BlockSpec(memory_space=pltpu.HBM)],
        out_specs=(vmem,) * 4,
        out_shape=(
            jax.ShapeDtypeStruct((GRP, 32, 2 * N), bf16),
            jax.ShapeDtypeStruct((1, 256), jnp.int32),
            jax.ShapeDtypeStruct((BEAMS, 4, 8, N), bf16),
            jax.ShapeDtypeStruct((BEAMS, 256, 2 * N), bf16),
        ),
        scratch_shapes=[
            pltpu.VMEM((BEAMS, 4, BLK, N), bf16),
            pltpu.VMEM((2 * N // 128, BLK + 8, 128), f32),
            pltpu.VMEM((256, N), bf16),
            pltpu.SemaphoreType.DMA((BEAMS,)),
        ],
        compiler_params=pltpu.CompilerParams(vmem_limit_bytes=46 << 20),
        name="front",
    )(small, volt)


def coarse_kernel(tail_ref, halo_ref, small_ref, wt_ref, filt_ref, out_ref, buf_ref, ext_ref):
    for b in range(BEAMS):
        for op in range(4):
            o, p = divmod(op, 2)
            for c in range(N // 128):
                lanes = pl.ds(c * 128, 128)
                slot = (b % 2) * 16 + op * 4 + c
                ext_ref[slot, 0:8, :] = tail_ref[b, op, :, lanes].astype(f32)
                ext_ref[slot, 8 : 8 + HALO, :] = halo_ref[b, op, :, lanes].astype(f32)
                acc = small_ref[0:1, lanes] * ext_ref[slot, 0:8, :]
                for tap in range(1, TAPS):
                    acc = acc + small_ref[tap : tap + 1, lanes] * ext_ref[slot, tap : tap + 8, :]
                buf_ref[b, (o + 1) * BLK - 8 : (o + 1) * BLK, p * N + c * 128 : p * N + (c + 1) * 128] = acc.astype(bf16)
        for h in range(2):
            half = slice(h * GRP // 2, (h + 1) * GRP // 2)
            res = lax.dot_general(
                wt_ref[half].reshape(256, 2 * N),
                buf_ref[b],
                (((1,), (1,)), ((), ())),
                preferred_element_type=f32,
            )
            out_ref[half, b] = (res * (N ** -0.5)).astype(bf16).reshape(GRP // 2, 32, 256)


def coarse(tail, halo, small, wt, filt):
    vmem = pl.BlockSpec(memory_space=pltpu.VMEM)
    return pl.pallas_call(
        coarse_kernel,
        in_specs=[vmem] * 5,
        out_specs=(vmem, vmem),
        out_shape=(
            jax.ShapeDtypeStruct((GRP, BEAMS, 32, 256), bf16),
            jax.ShapeDtypeStruct((BEAMS, 256, 2 * N), bf16),
        ),
        input_output_aliases={4: 1},
        scratch_shapes=[pltpu.VMEM((32, 16, 128), f32)],
        compiler_params=pltpu.CompilerParams(vmem_limit_bytes=46 << 20),
        name="coarse",
    )(tail, halo, small, wt, filt)


def fine_kernel(rate_ref, x_ref, first_ref, second_hbm, perm_ref, out_ref, second_ref, lhs_ref, mix_ref, pow_ref, pow2_ref, sem):
    load = pltpu.make_async_copy(second_hbm, second_ref, sem)
    load.start()

    def beam(b, carry):
        rows = pl.ds(pl.multiple_of(b * 16, 16), 16)
        x = x_ref[:, b].reshape(512, 256)
        for h in range(2):
            y = jnp.dot(first_ref[h * 256 : (h + 1) * 256], x, preferred_element_type=f32).astype(bf16)
            for f in range(8):
                for q in range(2):
                    part = y[(2 * f + q) * 16 : (2 * f + q + 1) * 16]
                    for o in range(2):
                        lhs_ref[8 * h + f, o, rows, q * BLK : (q + 1) * BLK] = part[:, o * BLK : (o + 1) * BLK]
        return carry

    lax.fori_loop(0, BEAMS, beam, 0, unroll=8)
    load.wait()
    for f in range(GRP):
        total = None
        for o in range(2):
            z = jnp.dot(lhs_ref[f, o], second_ref[f], preferred_element_type=f32)
            part = z[:, 0:BLK] * z[:, 0:BLK] + z[:, BLK : 2 * BLK] * z[:, BLK : 2 * BLK]
            total = part if total is None else total + part
        pow2_ref[f] = total * (1.0 / 8192.0)
    lane = lax.broadcasted_iota(jnp.int32, (16, 128), 1)

    def mix(b, carry):
        rows = pl.ds(pl.multiple_of(b * 16, 16), 16)
        for h in range(2):
            v = [pow2_ref[8 * h + i, rows, :] for i in range(8)]
            for bit in (1, 2, 4):
                odd = (lane // (16 * bit)) % 2 == 1
                v = [jnp.where(odd, v[(m + bit) % 8], v[m]) for m in range(8)]
            for m in range(8):
                mix_ref[(8 - m) % 8, rows, h * 128 : (h + 1) * 128] = v[m].astype(bf16)
        return carry

    lax.fori_loop(0, BEAMS, mix, 0, unroll=4)
    zero = jnp.zeros((128, 128), f32)
    for e in (0, 1, 18, 19, 20):
        pow_ref[e] = zero
    for m in range(8):
        spots = [h * BLK + 16 * ((p - m) % 8) for h in range(2) for p in range(8)]
        turned = jnp.concatenate([perm_ref[r : r + 16] for r in spots], axis=0)
        q = jnp.dot(mix_ref[m], turned, preferred_element_type=f32)
        for h in range(2):
            for b in range(BEAMS):
                tile = q[b * 16 : (b + 1) * 16, h * 128 : (h + 1) * 128]
                pow_ref[2 + 2 * m + h, pl.ds(b, 16, stride=8), :] = tile
    low_lane = lax.broadcasted_iota(jnp.int32, (8, 128), 1)
    step = lax.axis_index(("x", "zh"))
    own = lax.axis_index(("zl", "y", "core")) * 16

    def shift(pair, carry):
        both = []
        for e in range(2):
            ch = 2 * pair + e
            start = 256 + rate_ref[0, own + ch] * step
            base = lax.shift_right_logical(start, 7)
            off = start & 127
            rows = pl.ds(pl.multiple_of(ch * 8, 8), 8)
            last = low_lane >= off
            r = [pow_ref[base + k, rows, :] for k in range(19)]
            both.append([pltpu.roll(jnp.where(last, r[k], r[k + 1]), (128 - off) & 127, 1) for k in range(18)])
        rows = pl.ds(pl.multiple_of((pair % 2) * 16, 16), 16)
        tiles = [jnp.concatenate([both[0][k], both[1][k]], axis=0).astype(bf16) for k in range(18)]
        for x in range(4):
            for w in range(WIN // 128):
                out_ref[pair // 2, x, rows, w * 128 : (w + 1) * 128] = tiles[4 * x + w]
        return carry

    lax.fori_loop(0, 8, shift, 0, unroll=4)


def fine(rates, x, first, second, perm):
    vmem = pl.BlockSpec(memory_space=pltpu.VMEM)
    return pl.pallas_call(
        fine_kernel,
        in_specs=[
            pl.BlockSpec(memory_space=pltpu.SMEM),
            vmem,
            vmem,
            pl.BlockSpec(memory_space=pltpu.HBM),
            vmem,
        ],
        out_specs=vmem,
        out_shape=jax.ShapeDtypeStruct((4, 4, 32, WIN), bf16),
        scratch_shapes=[
            pltpu.VMEM((GRP, 256, 256), bf16),
            pltpu.VMEM((GRP, 2, 128, 256), bf16),
            pltpu.VMEM((8, 128, 256), bf16),
            pltpu.VMEM((21, 128, 128), f32),
            pltpu.VMEM((GRP, 128, 128), f32),
            pltpu.SemaphoreType.DMA,
        ],
        compiler_params=pltpu.CompilerParams(vmem_limit_bytes=50 << 20),
        name="fine",
    )(rates, x, first, second, perm)


def drift_kernel(x_ref, out_ref, sum_ref, stage_ref, sem):
    lane = lax.broadcasted_iota(jnp.int16, (16, 128), 1)

    def send(b, pair):
        part = pl.ds(pl.multiple_of(b * 64 + pair * 32, 32), 32)
        return pltpu.make_async_copy(stage_ref.at[part], out_ref.at[part], sem.at[pair, b])

    def body(pair, carry):
        rows = pl.ds(pl.multiple_of(pair * 16, 16), 16)
        for j in range(NDRIFT):
            acc = None
            for t in range(STEPS):
                base, off = divmod(j * t, 128)
                r = [x_ref[t % 4 * 4 + t // 4, rows, (base + k) * 128 : (base + k + 1) * 128] for k in range(5 if off else 4)]
                if off:
                    keep = lane >= jnp.int16(off)
                    r = [pltpu.roll(jnp.where(keep, r[k], r[k + 1]), 128 - off, 1) for k in range(4)]
                w = [r[k].astype(f32) for k in range(4)]
                acc = w if acc is None else [acc[k] + w[k] for k in range(4)]
            for k in range(4):
                done = acc[k] * (1.0 / STEPS)
                for e in range(2):
                    at = (2 * pair + e) * NDRIFT + j
                    sum_ref[k, pl.ds(at, 8, stride=64), :] = done[8 * e : 8 * e + 8]
        for b in range(BEAMS):
            part = pl.ds(pl.multiple_of(b * 64 + pair * 32, 32), 32)
            for k in range(4):
                stage_ref[part, k * 128 : (k + 1) * 128] = sum_ref[k, part, :]
            send(b, pair).start()
        return carry

    lax.fori_loop(0, 2, body, 0)
    for pair in range(2):
        for b in range(BEAMS):
            send(b, pair).wait()


def drift(x):
    return pl.pallas_call(
        drift_kernel,
        in_specs=[pl.BlockSpec(memory_space=pltpu.VMEM)],
        out_specs=pl.BlockSpec(memory_space=pltpu.HBM),
        out_shape=jax.ShapeDtypeStruct((BEAMS * 64, BINS), f32),
        scratch_shapes=[
            pltpu.VMEM((4, BEAMS * 64, 128), f32),
            pltpu.VMEM((BEAMS * 64, BINS), f32),
            pltpu.SemaphoreType.DMA((2, BEAMS)),
        ],
        compiler_params=pltpu.CompilerParams(vmem_limit_bytes=50 << 20),
        name="drift",
    )(x)


def shards(voltages, taps, busy_mask, drift_low):
    axes = ("x", "zh", "zl", "y", "core")
    devices = lax.axis_size(axes)
    head = lax.slice_in_dim(voltages, 0, HALO, axis=2)
    halo = lax.ppermute(head, axes, [(i + 1, i) for i in range(devices - 1)])
    first, second, perm = fine_tables()
    row = lax.broadcasted_iota(jnp.int32, (8, N), 0)
    extra = jnp.where(row == TAPS, busy_mask[None, :], drift_low[None, :]).astype(f32)
    small = jnp.where(row < TAPS, jnp.pad(taps, ((0, 4), (0, 0))), extra)
    wt, rates, tail, filt = front(small, voltages)
    blocks, _ = coarse(tail, halo, small, wt, filt)
    times = lax.all_to_all(blocks, ("zl", "y", "core"), split_axis=0, concat_axis=0, tiled=True)
    powers = fine(rates, times, jnp.asarray(first), jnp.asarray(second), jnp.asarray(perm))
    wins = lax.all_to_all(powers.reshape(16, 32, WIN), ("zh", "x"), split_axis=0, concat_axis=0, tiled=True)
    out = drift(wins)
    return out.reshape(BEAMS, 4, NDRIFT, BINS)


def solution(mesh):
    fold = Mesh(mesh.devices.reshape(4, 4, 2, 4, 2), ("x", "zh", "zl", "y", "core"))
    chan = ("zh", "zl", "y", "core")
    in_specs = (P(None, None, ("x",) + chan, None), P(), P(), P())
    out_specs = P(None, chan, None, "x")
    return jax.shard_map(shards, mesh=fold, in_specs=in_specs, out_specs=out_specs, check_vma=False)
```

```python
import math

import jax
import jax.numpy as jnp
import numpy as np
from jax import lax
from jax.experimental import pallas as pl
from jax.experimental.pallas import tpu as pltpu
from jax.sharding import Mesh, PartitionSpec as P

TAPS = 4
HALO = 4
NDRIFT = 16
N = 512
FINE = 2048
BEAMS = 8
STEPS = 16
BLK = 128
GRP = 16
WIN = 768
BINS = 512
f32 = jnp.float32
bf16 = jnp.bfloat16


def np_bf16(a):
    return np.asarray(a, np.float32).astype(jnp.bfloat16)


def fine_tables():
    k = np.arange(GRP)
    sent = k % 2 * 8 + k // 2 % 4 * 2 + k // 8
    ang = (k[:, None] * sent[None, :]) % GRP * (2.0 * math.pi / GRP)
    c, sn = np.cos(ang), np.sin(ang)
    eye = np.eye(16)
    first = np.zeros((GRP, 2, 16, GRP, 2, 16))
    for q, p, val in ((0, 0, c), (0, 1, sn), (1, 0, -sn), (1, 1, c)):
        first[:, q, :, :, p, :] = val[:, None, :, None] * eye[None, :, None, :]
    f1 = np.arange(GRP)
    lane = np.arange(BLK)
    block = (lane[None, :] // 16 - f1[:, None]) % 8
    f2 = block * 16 + lane[None, :] % 16
    j = np.arange(BLK)
    ang = (j[None, :, None] * (f1[:, None] + 16 * f2)[:, None, :]) % FINE * (2.0 * math.pi / FINE)
    c, sn = np.cos(ang), np.sin(ang)
    second = np.concatenate([np.concatenate([c, -sn], 2), np.concatenate([sn, c], 2)], 1)
    perm = np.zeros((256, 256))
    for h in range(2):
        perm[h * 128 + lane, 8 * h + lane // 16 + 16 * (lane % 16)] = 1.0
    return np_bf16(first.reshape(512, 512)), np_bf16(second), np_bf16(perm)


def cos_sin(phase):
    quarter = lax.shift_right_arithmetic(phase + 64, 7)
    x = (phase - quarter * 128).astype(f32) * (2.0 * math.pi / N)
    y = x * x
    c = 1.0 + y * (-0.5 + y * (1.0 / 24 + y * (-1.0 / 720 + y * (1.0 / 40320))))
    s = x * (1.0 + y * (-1.0 / 6 + y * (1.0 / 120 + y * (-1.0 / 5040 + y * (1.0 / 362880)))))
    swap = (quarter & 1) == 1
    cos = jnp.where(swap, s, c)
    sin = jnp.where(swap, c, s)
    cos = jnp.where(((quarter + 1) & 2) == 2, -cos, cos)
    sin = jnp.where((quarter & 2) == 2, -sin, sin)
    return cos, sin


def write_tables(small_ref, wt_ref, rate_ref, hit_ref):
    busy = small_ref[TAPS : TAPS + 1]
    row = lax.broadcasted_iota(jnp.int32, (N, N), 0)
    col = lax.broadcasted_iota(jnp.int32, (N, N), 1)
    upper = (row < col).astype(f32).astype(bf16)
    mask = jnp.broadcast_to(busy, (8, N))
    before = jnp.dot(mask.astype(bf16), upper, preferred_element_type=f32)[0:1].astype(jnp.int32)
    before = jnp.where(busy > 0.5, before, -1)
    for r0 in range(0, 256, 16):
        rp = r0 + lax.broadcasted_iota(jnp.int32, (16, N), 0)
        pos = lax.broadcasted_iota(jnp.int32, (16, N), 1)
        group = (rp // 16) % 2 * 8 + (rp // 32) % 4 * 2 + rp // 128
        hit = before == (rp // 4) % 4 * 64 + group * 4 + rp % 4
        hit_ref[r0 : r0 + 16] = hit.astype(f32).astype(bf16)
        chan = jnp.sum(jnp.where(hit, pos, 0), axis=1, keepdims=True)
        cos, sin = cos_sin((chan * pos[:, 0:BLK]) & (N - 1))
        for c in range(N // BLK):
            turns = (chan * c) & 3
            odd = (turns & 1) == 1
            cos_sign = jnp.where((turns == 1) | (turns == 2), -1.0, 1.0)
            sin_sign = jnp.where(turns >= 2, -1.0, 1.0)
            cc = jnp.where(odd, sin, cos) * cos_sign
            ss = jnp.where(odd, cos, sin) * sin_sign
            lanes = slice(c * BLK, (c + 1) * BLK)
            high = slice(N + c * BLK, N + (c + 1) * BLK)
            wt_ref[r0 // 16, 0:16, lanes] = cc.astype(bf16)
            wt_ref[r0 // 16, 0:16, high] = ss.astype(bf16)
            wt_ref[r0 // 16, 16:32, lanes] = (-ss).astype(bf16)
            wt_ref[r0 // 16, 16:32, high] = cc.astype(bf16)
    low = jnp.broadcast_to(small_ref[TAPS + 1 : TAPS + 2], (8, N)).astype(bf16)
    rate = lax.dot_general(low, hit_ref[...], (((1,), (1,)), ((), ())), preferred_element_type=f32)
    rate_ref[...] = rate[0:1].astype(jnp.int32)


def front_kernel(small_ref, v_ref, wt_ref, rate_ref, tail_ref, filt_ref, buf_ref, ext_ref, hit_ref, sem):
    def fetch(b):
        return pltpu.make_async_copy(v_ref.at[b], buf_ref.at[b], sem.at[b])

    for b in range(BEAMS):
        fetch(b).start()
    write_tables(small_ref, wt_ref, rate_ref, hit_ref)
    for e in range(2 * N // 128):
        ext_ref[e, BLK : BLK + 8, :] = jnp.zeros((8, 128), f32)

    def beam(b, carry):
        fetch(b).wait()
        tail_ref[b] = buf_ref[b, :, BLK - 8 : BLK, :]

        def body(o, inner):
            row = pl.multiple_of(o * BLK, BLK)
            for p in range(2):
                for c in range(N // 128):
                    e = p * (N // 128) + c
                    lanes = pl.ds(c * 128, 128)
                    main = buf_ref[b, 2 * o + p, :, lanes].astype(f32)
                    ext_ref[e, 0:BLK, :] = main
                    acc = small_ref[0:1, lanes] * main
                    for tap in range(1, TAPS):
                        acc = acc + small_ref[tap : tap + 1, lanes] * ext_ref[e, tap : tap + BLK, :]
                    filt_ref[b, pl.ds(row, BLK), e * 128 : (e + 1) * 128] = acc.astype(bf16)
            return inner

        return lax.fori_loop(0, 2, body, carry, unroll=2)

    lax.fori_loop(0, BEAMS, beam, 0)


def front(small, volt):
    vmem = pl.BlockSpec(memory_space=pltpu.VMEM)
    return pl.pallas_call(
        front_kernel,
        in_specs=[vmem, pl.BlockSpec(memory_space=pltpu.HBM)],
        out_specs=(vmem,) * 4,
        out_shape=(
            jax.ShapeDtypeStruct((GRP, 32, 2 * N), bf16),
            jax.ShapeDtypeStruct((1, 256), jnp.int32),
            jax.ShapeDtypeStruct((BEAMS, 4, 8, N), bf16),
            jax.ShapeDtypeStruct((BEAMS, 256, 2 * N), bf16),
        ),
        scratch_shapes=[
            pltpu.VMEM((BEAMS, 4, BLK, N), bf16),
            pltpu.VMEM((2 * N // 128, BLK + 8, 128), f32),
            pltpu.VMEM((256, N), bf16),
            pltpu.SemaphoreType.DMA((BEAMS,)),
        ],
        compiler_params=pltpu.CompilerParams(vmem_limit_bytes=46 << 20),
        name="front",
    )(small, volt)


def coarse_kernel(tail_ref, halo_ref, small_ref, wt_ref, filt_ref, out_ref, buf_ref, ext_ref):
    for b in range(BEAMS):
        for op in range(4):
            o, p = divmod(op, 2)
            for c in range(N // 128):
                lanes = pl.ds(c * 128, 128)
                slot = (b % 2) * 16 + op * 4 + c
                ext_ref[slot, 0:8, :] = tail_ref[b, op, :, lanes].astype(f32)
                ext_ref[slot, 8 : 8 + HALO, :] = halo_ref[b, op, :, lanes].astype(f32)
                acc = small_ref[0:1, lanes] * ext_ref[slot, 0:8, :]
                for tap in range(1, TAPS):
                    acc = acc + small_ref[tap : tap + 1, lanes] * ext_ref[slot, tap : tap + 8, :]
                buf_ref[b, (o + 1) * BLK - 8 : (o + 1) * BLK, p * N + c * 128 : p * N + (c + 1) * 128] = acc.astype(bf16)
        for h in range(2):
            half = slice(h * GRP // 2, (h + 1) * GRP // 2)
            res = lax.dot_general(
                wt_ref[half].reshape(256, 2 * N),
                buf_ref[b],
                (((1,), (1,)), ((), ())),
                preferred_element_type=f32,
            )
            out_ref[half, b] = (res * (N ** -0.5)).astype(bf16).reshape(GRP // 2, 32, 256)


def coarse(tail, halo, small, wt, filt):
    vmem = pl.BlockSpec(memory_space=pltpu.VMEM)
    return pl.pallas_call(
        coarse_kernel,
        in_specs=[vmem] * 5,
        out_specs=(vmem, vmem),
        out_shape=(
            jax.ShapeDtypeStruct((GRP, BEAMS, 32, 256), bf16),
            jax.ShapeDtypeStruct((BEAMS, 256, 2 * N), bf16),
        ),
        input_output_aliases={4: 1},
        scratch_shapes=[pltpu.VMEM((32, 16, 128), f32)],
        compiler_params=pltpu.CompilerParams(vmem_limit_bytes=46 << 20),
        name="coarse",
    )(tail, halo, small, wt, filt)


def fine_kernel(rate_ref, x_ref, first_ref, second_hbm, perm_ref, out_ref, second_ref, lhs_ref, mix_ref, pow_ref, pow2_ref, sem):
    load = pltpu.make_async_copy(second_hbm, second_ref, sem)
    load.start()

    def beam(b, carry):
        rows = pl.ds(pl.multiple_of(b * 16, 16), 16)
        x = x_ref[:, b].reshape(512, 256)
        for h in range(2):
            y = jnp.dot(first_ref[h * 256 : (h + 1) * 256], x, preferred_element_type=f32).astype(bf16)
            for f in range(8):
                for q in range(2):
                    part = y[(2 * f + q) * 16 : (2 * f + q + 1) * 16]
                    for o in range(2):
                        lhs_ref[8 * h + f, o, rows, q * BLK : (q + 1) * BLK] = part[:, o * BLK : (o + 1) * BLK]
        return carry

    lax.fori_loop(0, BEAMS, beam, 0, unroll=8)
    load.wait()
    for f in range(GRP):
        total = None
        for o in range(2):
            z = jnp.dot(lhs_ref[f, o], second_ref[f], preferred_element_type=f32)
            part = z[:, 0:BLK] * z[:, 0:BLK] + z[:, BLK : 2 * BLK] * z[:, BLK : 2 * BLK]
            total = part if total is None else total + part
        pow2_ref[f] = total * (1.0 / 8192.0)
    lane = lax.broadcasted_iota(jnp.int32, (16, 128), 1)

    def mix(b, carry):
        rows = pl.ds(pl.multiple_of(b * 16, 16), 16)
        for h in range(2):
            v = [pow2_ref[8 * h + i, rows, :] for i in range(8)]
            for bit in (1, 2, 4):
                odd = (lane // (16 * bit)) % 2 == 1
                v = [jnp.where(odd, v[(m + bit) % 8], v[m]) for m in range(8)]
            for m in range(8):
                mix_ref[(8 - m) % 8, rows, h * 128 : (h + 1) * 128] = v[m].astype(bf16)
        return carry

    lax.fori_loop(0, BEAMS, mix, 0, unroll=4)
    zero = jnp.zeros((128, 128), f32)
    for e in (0, 1, 18, 19, 20):
        pow_ref[e] = zero
    for m in range(8):
        spots = [h * BLK + 16 * ((p - m) % 8) for h in range(2) for p in range(8)]
        turned = jnp.concatenate([perm_ref[r : r + 16] for r in spots], axis=0)
        q = jnp.dot(mix_ref[m], turned, preferred_element_type=f32)
        for h in range(2):
            for b in range(BEAMS):
                tile = q[b * 16 : (b + 1) * 16, h * 128 : (h + 1) * 128]
                pow_ref[2 + 2 * m + h, pl.ds(b, 16, stride=8), :] = tile
    low_lane = lax.broadcasted_iota(jnp.int32, (8, 128), 1)
    step = lax.axis_index(("x", "zh"))
    own = lax.axis_index(("core", "y", "zl")) * 16

    def shift(pair, carry):
        both = []
        for e in range(2):
            ch = 2 * pair + e
            start = 256 + rate_ref[0, own + ch] * step
            base = lax.shift_right_logical(start, 7)
            off = start & 127
            rows = pl.ds(pl.multiple_of(ch * 8, 8), 8)
            last = low_lane >= off
            r = [pow_ref[base + k, rows, :] for k in range(19)]
            both.append([pltpu.roll(jnp.where(last, r[k], r[k + 1]), (128 - off) & 127, 1) for k in range(18)])
        rows = pl.ds(pl.multiple_of((pair % 2) * 16, 16), 16)
        tiles = [jnp.concatenate([both[0][k], both[1][k]], axis=0).astype(bf16) for k in range(18)]
        for x in range(4):
            for w in range(WIN // 128):
                out_ref[pair // 2, x, rows, w * 128 : (w + 1) * 128] = tiles[4 * x + w]
        return carry

    lax.fori_loop(0, 8, shift, 0, unroll=4)


def fine(rates, x, first, second, perm):
    vmem = pl.BlockSpec(memory_space=pltpu.VMEM)
    return pl.pallas_call(
        fine_kernel,
        in_specs=[
            pl.BlockSpec(memory_space=pltpu.SMEM),
            vmem,
            vmem,
            pl.BlockSpec(memory_space=pltpu.HBM),
            vmem,
        ],
        out_specs=vmem,
        out_shape=jax.ShapeDtypeStruct((4, 4, 32, WIN), bf16),
        scratch_shapes=[
            pltpu.VMEM((GRP, 256, 256), bf16),
            pltpu.VMEM((GRP, 2, 128, 256), bf16),
            pltpu.VMEM((8, 128, 256), bf16),
            pltpu.VMEM((21, 128, 128), f32),
            pltpu.VMEM((GRP, 128, 128), f32),
            pltpu.SemaphoreType.DMA,
        ],
        compiler_params=pltpu.CompilerParams(vmem_limit_bytes=50 << 20),
        name="fine",
    )(rates, x, first, second, perm)


def drift_kernel(x_ref, out_ref, sum_ref, stage_ref, sem):
    lane = lax.broadcasted_iota(jnp.int16, (16, 128), 1)

    def send(b, pair):
        part = pl.ds(pl.multiple_of(b * 64 + pair * 32, 32), 32)
        return pltpu.make_async_copy(stage_ref.at[part], out_ref.at[part], sem.at[pair, b])

    def body(pair, carry):
        rows = pl.ds(pl.multiple_of(pair * 16, 16), 16)
        for j in range(NDRIFT):
            acc = None
            for t in range(STEPS):
                base, off = divmod(j * t, 128)
                r = [x_ref[t % 4 * 4 + t // 4, rows, (base + k) * 128 : (base + k + 1) * 128] for k in range(5 if off else 4)]
                if off:
                    keep = lane >= jnp.int16(off)
                    r = [pltpu.roll(jnp.where(keep, r[k], r[k + 1]), 128 - off, 1) for k in range(4)]
                w = [r[k].astype(f32) for k in range(4)]
                acc = w if acc is None else [acc[k] + w[k] for k in range(4)]
            for k in range(4):
                done = acc[k] * (1.0 / STEPS)
                for e in range(2):
                    at = (2 * pair + e) * NDRIFT + j
                    sum_ref[k, pl.ds(at, 8, stride=64), :] = done[8 * e : 8 * e + 8]
        for b in range(BEAMS):
            part = pl.ds(pl.multiple_of(b * 64 + pair * 32, 32), 32)
            for k in range(4):
                stage_ref[part, k * 128 : (k + 1) * 128] = sum_ref[k, part, :]
            send(b, pair).start()
        return carry

    lax.fori_loop(0, 2, body, 0)
    for pair in range(2):
        for b in range(BEAMS):
            send(b, pair).wait()


def drift(x):
    return pl.pallas_call(
        drift_kernel,
        in_specs=[pl.BlockSpec(memory_space=pltpu.VMEM)],
        out_specs=pl.BlockSpec(memory_space=pltpu.HBM),
        out_shape=jax.ShapeDtypeStruct((BEAMS * 64, BINS), f32),
        scratch_shapes=[
            pltpu.VMEM((4, BEAMS * 64, 128), f32),
            pltpu.VMEM((BEAMS * 64, BINS), f32),
            pltpu.SemaphoreType.DMA((2, BEAMS)),
        ],
        compiler_params=pltpu.CompilerParams(vmem_limit_bytes=50 << 20),
        name="drift",
    )(x)


def shards(voltages, taps, busy_mask, drift_low):
    axes = ("x", "zh", "zl", "y", "core")
    devices = lax.axis_size(axes)
    head = lax.slice_in_dim(voltages, 0, HALO, axis=2)
    halo = lax.ppermute(head, axes, [(i + 1, i) for i in range(devices - 1)])
    first, second, perm = fine_tables()
    row = lax.broadcasted_iota(jnp.int32, (8, N), 0)
    extra = jnp.where(row == TAPS, busy_mask[None, :], drift_low[None, :]).astype(f32)
    small = jnp.where(row < TAPS, jnp.pad(taps, ((0, 4), (0, 0))), extra)
    wt, rates, tail, filt = front(small, voltages)
    blocks, _ = coarse(tail, halo, small, wt, filt)
    times = lax.all_to_all(blocks, ("core", "y", "zl"), split_axis=0, concat_axis=0, tiled=True)
    powers = fine(rates, times, jnp.asarray(first), jnp.asarray(second), jnp.asarray(perm))
    wins = lax.all_to_all(powers.reshape(16, 32, WIN), ("zh", "x"), split_axis=0, concat_axis=0, tiled=True)
    out = drift(wins)
    return out.reshape(BEAMS, 4, NDRIFT, BINS)


def solution(mesh):
    fold = Mesh(mesh.devices.reshape(4, 4, 2, 4, 2), ("x", "zh", "zl", "y", "core"))
    chan = ("zh", "zl", "y", "core")
    in_specs = (P(None, None, ("x",) + chan, None), P(), P(), P())
    out_specs = P(None, chan, None, "x")
    return jax.shard_map(shards, mesh=fold, in_specs=in_specs, out_specs=out_specs, check_vma=False)
```
